16 devices in a mesh: fsdp: 16 (over z, y, x, core).
Axes of the slice: x: 2, y: 2, z: 2, core: 2. Of those that a mesh axis runs over, the one named last changes fastest.
Arguments:
- grad_mat: bfloat16 [16, 21233664], P('fsdp')
- grad_vec: bfloat16 [16, 14336], P('fsdp')
- master_mat: float32 [21233664], P('fsdp')
- moment_mat: float32 [21233664], P('fsdp')
- second_mat: float32 [21233664], P('fsdp')
- master_vec: float32 [14336], P('fsdp')
- moment_vec: float32 [14336], P('fsdp')
- second_vec: float32 [14336], P('fsdp')
Outputs:
- output 1: float32 [21233664], P('fsdp')
- output 2: float32 [21233664], P('fsdp')
- output 3: float32 [21233664], P('fsdp')
- output 4: float32 [14336], P('fsdp')
- output 5: float32 [14336], P('fsdp')
- output 6: float32 [14336], P('fsdp')
- output 7: bfloat16 [21233664], replicated
- output 8: bfloat16 [14336], replicated
All inputs are finite; a program needn't handle non-finite values.
Results may differ from the reference program's by a relative error of at most 0.001.
Values are sent between devices in bfloat16 or wider.
A program may use at most 1 GiB of HBM per device.

```python
import jax
import jax.numpy as jnp
from jax import lax

D = 576
HEADS = 9
KV_HEADS = 3
HEAD = 64
FF = 1536
LAYERS = 6
GROUP = 16
NM_PAD = 21233664
NV_PAD = 14336
STEP = 4

Q_OUT = HEADS * HEAD
KV_OUT = KV_HEADS * HEAD
MAT_COUNT = LAYERS * (2 * D * Q_OUT + 2 * D * KV_OUT + 3 * D * FF)
VEC_COUNT = LAYERS * (Q_OUT + 2 * KV_OUT + 2 * D)
GRAD_UNIT = (MAT_COUNT + VEC_COUNT) ** -0.5
TARGET_NORM = 3.0
LEARN_RATE = 1e-3
BETA_ONE = 0.9
BETA_TWO = 0.999
ADAM_EPS = 1e-8
DECAY = 0.01
NORM_EPS = 1e-6
FIX_ONE = 1.0 - BETA_ONE ** STEP
FIX_TWO = 1.0 - BETA_TWO ** STEP


def pad_flat(flat, total):
    return jnp.pad(flat, (0, total - flat.shape[0]))


def layer_draw(key, pieces):
    sub_keys = jax.random.split(key, len(pieces))
    drawn = [jax.random.normal(sub_key, (LAYERS, length), jnp.float32) * scale + offset
             for sub_key, (length, scale, offset) in zip(sub_keys, pieces)]
    return jnp.concatenate(drawn, axis=1).reshape(-1)


def grad_rows(key, total, valid):
    keep = jnp.arange(total) < valid
    scale = TARGET_NORM * GRAD_UNIT * GROUP ** -0.5

    def one_row(row):
        noise = jax.random.normal(jax.random.fold_in(key, row), (total,), jnp.float32)
        return jnp.where(keep, noise * scale, 0.0).astype(jnp.bfloat16)

    return lax.map(one_row, jnp.arange(GROUP))


def moment_draw(key, total, valid):
    keep = jnp.arange(total) < valid
    noise = jax.random.normal(key, (total,), jnp.float32)
    return jnp.where(keep, 0.1 * GRAD_UNIT * noise, 0.0)


def second_draw(key, total, valid):
    keep = jnp.arange(total) < valid
    noise = jax.random.normal(key, (total,), jnp.float32)
    return jnp.where(keep, 0.003 * GRAD_UNIT ** 2 * (noise * noise + 0.5), 0.0)


def setup_inputs(seed: int = 0) -> dict:
    keys = jax.random.split(jax.random.key(seed), 8)
    mat_pieces = [(D * Q_OUT, D ** -0.5, 0.0), (D * KV_OUT, D ** -0.5, 0.0), (D * KV_OUT, D ** -0.5, 0.0),
                  (Q_OUT * D, Q_OUT ** -0.5, 0.0), (D * FF, D ** -0.5, 0.0), (D * FF, D ** -0.5, 0.0),
                  (FF * D, FF ** -0.5, 0.0)]
    vec_pieces = [(Q_OUT, 0.5, 0.0), (KV_OUT, 0.5, 0.0), (KV_OUT, 0.5, 0.0), (D, 0.2, 1.0), (D, 0.2, 1.0)]
    return {
        'grad_mat': grad_rows(keys[0], NM_PAD, MAT_COUNT),
        'grad_vec': grad_rows(keys[1], NV_PAD, VEC_COUNT),
        'master_mat': pad_flat(layer_draw(keys[2], mat_pieces), NM_PAD),
        'moment_mat': moment_draw(keys[3], NM_PAD, MAT_COUNT),
        'second_mat': second_draw(keys[4], NM_PAD, MAT_COUNT),
        'master_vec': pad_flat(layer_draw(keys[5], vec_pieces), NV_PAD),
        'moment_vec': moment_draw(keys[6], NV_PAD, VEC_COUNT),
        'second_vec': second_draw(keys[7], NV_PAD, VEC_COUNT),
    }


def row_total(grad_block):
    def add_row(running, row_vals):
        return running + row_vals.astype(jnp.float32), None

    total, _ = lax.scan(add_row, jnp.zeros(grad_block.shape[1:], jnp.float32), grad_block)
    return total


def adam_update(grad_sum, clip_coef, master, moment, second, decay):
    clip_grad = clip_coef * grad_sum
    new_moment = BETA_ONE * moment + (1.0 - BETA_ONE) * clip_grad
    new_second = BETA_TWO * second + (1.0 - BETA_TWO) * clip_grad * clip_grad
    step_dir = (new_moment / FIX_ONE) / (jnp.sqrt(new_second / FIX_TWO) + ADAM_EPS)
    new_master = master - LEARN_RATE * (step_dir + decay * master)
    return new_master, new_moment, new_second


def reference(grad_mat, grad_vec, master_mat, moment_mat, second_mat, master_vec, moment_vec, second_vec):
    sum_mat = row_total(grad_mat)
    sum_vec = row_total(grad_vec)
    total_norm = jnp.sqrt(jnp.sum(sum_mat * sum_mat) + jnp.sum(sum_vec * sum_vec))
    clip_coef = jnp.minimum(1.0, 1.0 / (total_norm + NORM_EPS))
    mat_out = adam_update(sum_mat, clip_coef, master_mat, moment_mat, second_mat, DECAY)
    vec_out = adam_update(sum_vec, clip_coef, master_vec, moment_vec, second_vec, 0.0)
    return (mat_out[0], mat_out[1], mat_out[2], vec_out[0], vec_out[1], vec_out[2],
            mat_out[0].astype(jnp.bfloat16), vec_out[0].astype(jnp.bfloat16))
```

```python
import functools

import jax
import jax.numpy as jnp
from jax import lax
from jax.experimental import pallas as pl
from jax.experimental.pallas import tpu as pltpu
from jax.sharding import PartitionSpec as P

STEP = 4
LEARN_RATE = 1e-3
BETA_ONE = 0.9
BETA_TWO = 0.999
ADAM_EPS = 1e-8
DECAY = 0.01
NORM_EPS = 1e-6
FIX_ONE = 1.0 - BETA_ONE ** STEP
FIX_TWO = 1.0 - BETA_TWO ** STEP

MESH = pl.DeviceIdType.MESH
LANES = 128
SLOTS = 3
STEPS = (2, 4, 8)
F32 = jnp.float32
BF16 = jnp.bfloat16


def adam_update(grad_sum, clip_coef, master, moment, second, decay):
    clip_grad = clip_coef * grad_sum
    new_moment = BETA_ONE * moment + (1.0 - BETA_ONE) * clip_grad
    new_second = BETA_TWO * second + (1.0 - BETA_TWO) * clip_grad * clip_grad
    step_dir = (new_moment / FIX_ONE) / (jnp.sqrt(new_second / FIX_TWO) + ADAM_EPS)
    new_master = master - LEARN_RATE * (step_dir + decay * master)
    return new_master, new_moment, new_second


def bit_of(index, stride):
    return lax.rem(lax.div(index, stride), 2)


def across(index, stride):
    return index + stride * (1 - 2 * bit_of(index, stride))


def reduce_kernel(chunks, rows, grad, gvec, total_out, vec_out, clip_out,
                  raw, packed, recv_a, send_b, keep_b, recv_b, send_c, keep_c, recv_c,
                  vec_in, square, square_in,
                  raw_sem, send_a_sem, recv_a_sem, send_b_sem, recv_b_sem, send_c_sem, recv_c_sem,
                  small_send, small_recv, free_sem):
    me = lax.axis_index('fsdp')
    core = bit_of(me, 1)
    group = 16

    barrier = pltpu.get_barrier_semaphore()
    for k in range(1, group):
        pl.semaphore_signal(barrier, inc=1, device_id=(lax.rem(me + k, group),), device_id_type=MESH)
    pl.semaphore_wait(barrier, group - 1)

    dims = [tuple(STEPS[(c + k) % 3] for k in range(3)) for c in range(3)]

    def load(c, t):
        slot = lax.rem(t + c, 2)
        return pltpu.make_async_copy(grad.at[:, c, t], raw.at[slot], raw_sem.at[slot])

    def peers(c):
        d1 = dims[c][0]
        other = across(me, d1)
        return ((across(me, 1), bit_of(me, d1), 1 - core),
                (other, 1 - bit_of(me, d1), core),
                (across(other, 1), 1 - bit_of(me, d1), 1 - core))

    def copy_a(c, t, j):
        device, d1_bit, core_bit = peers(c)[j]
        ps, rs = lax.rem(t, 2), lax.rem(t, SLOTS)
        return pltpu.make_async_remote_copy(
            src_ref=packed.at[c, ps, 2 * d1_bit + core_bit], dst_ref=recv_a.at[c, rs, j],
            send_sem=send_a_sem.at[c, ps, j], recv_sem=recv_a_sem.at[c, rs, j],
            device_id=(device,), device_id_type=MESH)

    def copy_b(c, t):
        s = lax.rem(t, 2)
        return pltpu.make_async_remote_copy(
            src_ref=send_b.at[c, s], dst_ref=recv_b.at[c, t],
            send_sem=send_b_sem.at[c, s], recv_sem=recv_b_sem.at[c, t],
            device_id=(across(me, dims[c][1]),), device_id_type=MESH)

    def copy_c(c, t):
        s = lax.rem(t, 2)
        return pltpu.make_async_remote_copy(
            src_ref=send_c.at[c, s], dst_ref=recv_c.at[c, t],
            send_sem=send_c_sem.at[c, s], recv_sem=recv_c_sem.at[c, t],
            device_id=(across(me, dims[c][2]),), device_id_type=MESH)

    blk = 96
    blocks = rows // blk

    def pack_and_send(c, t):
        load(c, t).wait()
        ps = lax.rem(t, 2)
        rs = lax.rem(t + c, 2)

        @pl.when(t >= 2)
        def _():
            for j in range(3):
                copy_a(c, t - 2, j).wait_send()

        d1, d2, d3 = dims[c]
        for share in range(group):
            bits = [(share // d) % 2 for d in (d1, 1, d2, d3)]
            quarter, part = 2 * bits[0] + bits[1], 2 * bits[2] + bits[3]

            def body(b, carry):
                start = pl.multiple_of(b * blk, blk)
                flat = raw[rs, share, :, pl.ds(pl.multiple_of(b * blk * LANES, blk * LANES), blk * LANES)]
                packed[c, ps, quarter, part, pl.ds(start, blk), :] = flat.reshape(blk, LANES)
                return carry

            lax.fori_loop(0, blocks, body, 0)

        @pl.when(t >= SLOTS)
        def _():
            for j in range(3):
                pl.semaphore_wait(free_sem.at[c, j], 1)

        for j in range(3):
            copy_a(c, t, j).start()

    def sum_a(c, t):
        ps, rs = lax.rem(t, 2), lax.rem(t, SLOTS)
        d1, d2, d3 = dims[c]
        mine = 2 * bit_of(me, d1) + core
        for j in range(3):
            copy_a(c, t, j).wait_recv()

        @pl.when(t >= 2)
        def _():
            copy_b(c, t - 2).wait_send()

        s = lax.rem(t, 2)
        for target, half in ((send_b, 1 - bit_of(me, d2)), (keep_b, bit_of(me, d2))):
            for k in range(2):
                part = 2 * half + k

                def body(b, carry):
                    here = pl.ds(pl.multiple_of(b * blk, blk), blk)
                    one = packed[c, ps, mine, part, here, :].astype(F32)
                    two = recv_a[c, rs, 0, part, here, :].astype(F32)
                    three = recv_a[c, rs, 1, part, here, :].astype(F32)
                    four = recv_a[c, rs, 2, part, here, :].astype(F32)
                    target[c, s, k, here, :] = (one + two) + (three + four)
                    return carry

                lax.fori_loop(0, blocks, body, 0)
            if target is send_b:
                copy_b(c, t).start()

        @pl.when(t + SLOTS < chunks)
        def _():
            for j in range(3):
                pl.semaphore_signal(free_sem.at[c, j], inc=1, device_id=(peers(c)[j][0],), device_id_type=MESH)

    def sum_b(c, t):
        d3 = dims[c][2]
        copy_b(c, t).wait_recv()

        @pl.when(t >= 2)
        def _():
            copy_c(c, t - 2).wait_send()

        s = lax.rem(t, 2)
        for target, k in ((send_c, 1 - bit_of(me, d3)), (keep_c, bit_of(me, d3))):
            def body(b, carry):
                here = pl.ds(pl.multiple_of(b * blk, blk), blk)
                target[c, s, here, :] = keep_b[c, s, k, here, :] + recv_b[c, t, k, here, :]
                return carry

            lax.fori_loop(0, blocks, body, 0)
            if target is send_c:
                copy_c(c, t).start()

    def sum_c(c, t):
        copy_c(c, t).wait_recv()
        s = lax.rem(t, 2)

        def body(b, running):
            here = pl.ds(pl.multiple_of(b * blk, blk), blk)
            there = pl.ds(pl.multiple_of((c * chunks + t) * rows + b * blk, blk), blk)
            total = keep_c[c, s, here, :] + recv_c[c, t, here, :]
            total_out[there, :] = total
            return running + jnp.sum((total * total).reshape(blk // 8, 8, LANES), axis=0)

        square[...] += lax.fori_loop(0, blocks, body, jnp.zeros((8, LANES), F32))

    def small_copy(src, dst, k, sem):
        return pltpu.make_async_remote_copy(
            src_ref=src, dst_ref=dst, send_sem=small_send.at[sem, k], recv_sem=small_recv.at[sem, k],
            device_id=(lax.rem(me + k, group),), device_id_type=MESH)

    def vec_copy(k):
        return small_copy(gvec.at[lax.rem(me + k, group)], vec_in.at[k], k, 0)

    def square_copy(k):
        return small_copy(square, square_in.at[k], k, 1)

    square[...] = jnp.zeros_like(square)
    for c in range(2):
        load(c, 0).start()
    for c in range(3):
        pack_and_send(c, 0)
        load((c + 2) % 3, (c + 2) // 3).start()
    for k in range(1, group):
        vec_copy(k).start()

    for c in range(3):
        pack_and_send(c, 1)
        load((c + 2) % 3, 1 + (c + 2) // 3).start()

    def tick(u, carry):
        for c in range(3):
            @pl.when(u < chunks)
            def _():
                sum_a(c, u)
        for c in range(3):
            @pl.when((u >= 1) & (u < chunks + 1))
            def _():
                sum_b(c, u - 1)
        for c in range(3):
            @pl.when(u >= 2)
            def _():
                sum_c(c, u - 2)
        for c in range(3):
            @pl.when(u + 2 < chunks)
            def _():
                pack_and_send(c, u + 2)

            nc, nt = (c + 2) % 3, u + 2 + (c + 2) // 3

            @pl.when(nt < chunks)
            def _():
                load(nc, nt).start()
        return carry

    lax.fori_loop(0, chunks + 2, tick, 0)

    vec_sum = gvec[me].astype(F32)
    for k in range(1, group):
        vec_copy(k).wait()
        vec_sum = vec_sum + vec_in[k].astype(F32)
    vec_out[...] = vec_sum
    square[0:1, :] += sum((vec_sum * vec_sum)[:, LANES * k:LANES * (k + 1)] for k in range(vec_sum.shape[1] // LANES))

    for k in range(1, group):
        square_copy(k).start()
    whole = square[...]
    for k in range(1, group):
        square_copy(k).wait_recv()
        whole = whole + square_in[k]
    for k in range(1, group):
        square_copy(k).wait_send()
    norm = jnp.sqrt(jnp.sum(whole, keepdims=True))
    clip_out[...] = jnp.broadcast_to(jnp.minimum(1.0, 1.0 / (norm + NORM_EPS)), clip_out.shape)

    for c in range(3):
        for t in range(chunks - 2, chunks):
            for j in range(3):
                copy_a(c, t, j).wait_send()
            copy_b(c, t).wait_send()
            copy_c(c, t).wait_send()


def reduce_share(grad_mat, grad_vec, group, chunks):
    share_rows = grad_mat.shape[1] // group // LANES
    rows = share_rows // (3 * chunks)
    vec_share = grad_vec.shape[1] // group
    grad = grad_mat.reshape(group, 3, chunks, 1, rows * LANES)
    gvec = grad_vec.reshape(group, 1, vec_share)
    vmem = pl.BlockSpec(memory_space=pltpu.VMEM)
    dma = pltpu.SemaphoreType.DMA
    total, vec, clip = pl.pallas_call(
        functools.partial(reduce_kernel, chunks, rows),
        out_shape=(jax.ShapeDtypeStruct((share_rows, LANES), F32),
                   jax.ShapeDtypeStruct((1, vec_share), F32),
                   jax.ShapeDtypeStruct((8, LANES), F32)),
        in_specs=[pl.BlockSpec(memory_space=pl.ANY), vmem],
        out_specs=(vmem, vmem, vmem),
        scratch_shapes=[
            pltpu.VMEM((2, group, 1, rows * LANES), BF16),
            pltpu.VMEM((3, 2, 4, 4, rows, LANES), BF16),
            pltpu.VMEM((3, SLOTS, 3, 4, rows, LANES), BF16),
            pltpu.VMEM((3, 2, 2, rows, LANES), F32),
            pltpu.VMEM((3, 2, 2, rows, LANES), F32),
            pltpu.VMEM((3, chunks, 2, rows, LANES), F32),
            pltpu.VMEM((3, 2, rows, LANES), F32),
            pltpu.VMEM((3, 2, rows, LANES), F32),
            pltpu.VMEM((3, chunks, rows, LANES), F32),
            pltpu.VMEM((group, 1, vec_share), BF16),
            pltpu.VMEM((8, LANES), F32),
            pltpu.VMEM((group, 8, LANES), F32),
            dma((2,)),
            dma((3, 2, 3)), dma((3, SLOTS, 3)),
            dma((3, 2)), dma((3, chunks)),
            dma((3, 2)), dma((3, chunks)),
            dma((2, group)), dma((2, group)),
            pltpu.SemaphoreType.REGULAR((3, 3)),
        ],
        compiler_params=pltpu.CompilerParams(collective_id=0, has_side_effects=True, vmem_limit_bytes=60 * 1024 * 1024),
        name='reduce_share',
    )(grad, gvec)
    return total.reshape(-1), vec.reshape(-1), clip[0, 0]


def solution(mesh):
    group = mesh.shape['fsdp']

    def local_step(grad_mat, grad_vec, master_mat, moment_mat, second_mat, master_vec, moment_vec, second_vec):
        sum_mat, sum_vec, clip_coef = reduce_share(grad_mat, grad_vec, group, 12)
        new_mat = adam_update(sum_mat, clip_coef, master_mat, moment_mat, second_mat, DECAY)
        new_vec = adam_update(sum_vec, clip_coef, master_vec, moment_vec, second_vec, 0.0)
        weights_mat = lax.all_gather(new_mat[0].astype(jnp.bfloat16), 'fsdp', tiled=True)
        weights_vec = lax.all_gather(new_vec[0].astype(jnp.bfloat16), 'fsdp', tiled=True)
        return new_mat + new_vec + (weights_mat, weights_vec)

    row_spec = P('fsdp', None)
    flat_spec = P('fsdp')
    whole_spec = P()
    return jax.shard_map(local_step, mesh=mesh,
                         in_specs=(row_spec, row_spec) + (flat_spec,) * 6,
                         out_specs=(flat_spec,) * 6 + (whole_spec, whole_spec),
                         check_vma=False)
```

```python
import functools

import jax
import jax.numpy as jnp
from jax import lax
from jax.experimental import pallas as pl
from jax.experimental.pallas import tpu as pltpu
from jax.sharding import PartitionSpec as P

STEP = 4
LEARN_RATE = 1e-3
BETA_ONE = 0.9
BETA_TWO = 0.999
ADAM_EPS = 1e-8
DECAY = 0.01
NORM_EPS = 1e-6
FIX_ONE = 1.0 - BETA_ONE ** STEP
FIX_TWO = 1.0 - BETA_TWO ** STEP

MESH = pl.DeviceIdType.MESH
LANES = 128
SLOTS = 3
STEPS = (2, 4, 8)
F32 = jnp.float32
BF16 = jnp.bfloat16


def adam_update(grad_sum, clip_coef, master, moment, second, decay):
    clip_grad = clip_coef * grad_sum
    new_moment = BETA_ONE * moment + (1.0 - BETA_ONE) * clip_grad
    new_second = BETA_TWO * second + (1.0 - BETA_TWO) * clip_grad * clip_grad
    step_dir = (new_moment / FIX_ONE) / (jnp.sqrt(new_second / FIX_TWO) + ADAM_EPS)
    new_master = master - LEARN_RATE * (step_dir + decay * master)
    return new_master, new_moment, new_second


def bit_of(index, stride):
    return lax.rem(lax.div(index, stride), 2)


def across(index, stride):
    return index + stride * (1 - 2 * bit_of(index, stride))


def reduce_kernel(chunks, rows, grad, gvec, total_out, vec_out, clip_out,
                  raw, packed, recv_a, send_b, keep_b, recv_b, send_c, keep_c, recv_c,
                  vec_in, square, square_in,
                  raw_sem, send_a_sem, recv_a_sem, send_b_sem, recv_b_sem, send_c_sem, recv_c_sem,
                  small_send, small_recv, free_sem):
    me = lax.axis_index('fsdp')
    core = bit_of(me, 1)
    group = 16

    barrier = pltpu.get_barrier_semaphore()
    for k in range(1, group):
        pl.semaphore_signal(barrier, inc=1, device_id=(lax.rem(me + k, group),), device_id_type=MESH)
    pl.semaphore_wait(barrier, group - 1)

    dims = [tuple(STEPS[(c + k) % 3] for k in range(3)) for c in range(3)]

    def load(c, t):
        slot = lax.rem(t + c, 2)
        return pltpu.make_async_copy(grad.at[:, c, t], raw.at[slot], raw_sem.at[slot])

    def peers(c):
        d1 = dims[c][0]
        other = across(me, d1)
        return ((across(me, 1), bit_of(me, d1), 1 - core),
                (other, 1 - bit_of(me, d1), core),
                (across(other, 1), 1 - bit_of(me, d1), 1 - core))

    def copy_a(c, t, j):
        device, d1_bit, core_bit = peers(c)[j]
        ps, rs = lax.rem(t, 2), lax.rem(t, SLOTS)
        return pltpu.make_async_remote_copy(
            src_ref=packed.at[c, ps, 2 * d1_bit + core_bit], dst_ref=recv_a.at[c, rs, j],
            send_sem=send_a_sem.at[c, ps, j], recv_sem=recv_a_sem.at[c, rs, j],
            device_id=(device,), device_id_type=MESH)

    def copy_b(c, t):
        s = lax.rem(t, 2)
        return pltpu.make_async_remote_copy(
            src_ref=send_b.at[c, s], dst_ref=recv_b.at[c, t],
            send_sem=send_b_sem.at[c, s], recv_sem=recv_b_sem.at[c, t],
            device_id=(across(me, dims[c][1]),), device_id_type=MESH)

    def copy_c(c, t):
        s = lax.rem(t, 2)
        return pltpu.make_async_remote_copy(
            src_ref=send_c.at[c, s], dst_ref=recv_c.at[c, t],
            send_sem=send_c_sem.at[c, s], recv_sem=recv_c_sem.at[c, t],
            device_id=(across(me, dims[c][2]),), device_id_type=MESH)

    blk = 96
    blocks = rows // blk

    def pack_and_send(c, t):
        load(c, t).wait()
        ps = lax.rem(t, 2)
        rs = lax.rem(t + c, 2)

        @pl.when(t >= 2)
        def _():
            for j in range(3):
                copy_a(c, t - 2, j).wait_send()

        d1, d2, d3 = dims[c]
        for share in range(group):
            bits = [(share // d) % 2 for d in (d1, 1, d2, d3)]
            quarter, part = 2 * bits[0] + bits[1], 2 * bits[2] + bits[3]

            def body(b, carry):
                start = pl.multiple_of(b * blk, blk)
                flat = raw[rs, share, :, pl.ds(pl.multiple_of(b * blk * LANES, blk * LANES), blk * LANES)]
                packed[c, ps, quarter, part, pl.ds(start, blk), :] = flat.reshape(blk, LANES)
                return carry

            lax.fori_loop(0, blocks, body, 0)

        @pl.when(t >= SLOTS)
        def _():
            for j in range(3):
                pl.semaphore_wait(free_sem.at[c, j], 1)

        for j in range(3):
            copy_a(c, t, j).start()

    def sum_a(c, t):
        ps, rs = lax.rem(t, 2), lax.rem(t, SLOTS)
        d1, d2, d3 = dims[c]
        mine = 2 * bit_of(me, d1) + core
        for j in range(3):
            copy_a(c, t, j).wait_recv()

        @pl.when(t >= 2)
        def _():
            copy_b(c, t - 2).wait_send()

        s = lax.rem(t, 2)
        for target, half in ((send_b, 1 - bit_of(me, d2)), (keep_b, bit_of(me, d2))):
            for k in range(2):
                part = 2 * half + k

                def body(b, carry):
                    here = pl.ds(pl.multiple_of(b * blk, blk), blk)
                    one = packed[c, ps, mine, part, here, :].astype(F32)
                    two = recv_a[c, rs, 0, part, here, :].astype(F32)
                    three = recv_a[c, rs, 1, part, here, :].astype(F32)
                    four = recv_a[c, rs, 2, part, here, :].astype(F32)
                    target[c, s, k, here, :] = (one + two) + (three + four)
                    return carry

                lax.fori_loop(0, blocks, body, 0)
            if target is send_b:
                copy_b(c, t).start()

        @pl.when(t + SLOTS < chunks)
        def _():
            for j in range(3):
                pl.semaphore_signal(free_sem.at[c, j], inc=1, device_id=(peers(c)[j][0],), device_id_type=MESH)

    def sum_b(c, t):
        d3 = dims[c][2]
        copy_b(c, t).wait_recv()

        @pl.when(t >= 2)
        def _():
            copy_c(c, t - 2).wait_send()

        s = lax.rem(t, 2)
        for target, k in ((send_c, 1 - bit_of(me, d3)), (keep_c, bit_of(me, d3))):
            def body(b, carry):
                here = pl.ds(pl.multiple_of(b * blk, blk), blk)
                target[c, s, here, :] = keep_b[c, s, k, here, :] + recv_b[c, t, k, here, :]
                return carry

            lax.fori_loop(0, blocks, body, 0)
            if target is send_c:
                copy_c(c, t).start()

    def sum_c(c, t):
        copy_c(c, t).wait_recv()
        s = lax.rem(t, 2)

        def body(b, running):
            here = pl.ds(pl.multiple_of(b * blk, blk), blk)
            there = pl.ds(pl.multiple_of((c * chunks + t) * rows + b * blk, blk), blk)
            total = keep_c[c, s, here, :] + recv_c[c, t, here, :]
            total_out[there, :] = total
            return running + jnp.sum((total * total).reshape(blk // 8, 8, LANES), axis=0)

        square[...] += lax.fori_loop(0, blocks, body, jnp.zeros((8, LANES), F32))

    def small_copy(src, dst, k, sem):
        return pltpu.make_async_remote_copy(
            src_ref=src, dst_ref=dst, send_sem=small_send.at[sem, k], recv_sem=small_recv.at[sem, k],
            device_id=(lax.rem(me + k, group),), device_id_type=MESH)

    def vec_copy(k):
        return small_copy(gvec.at[lax.rem(me + k, group)], vec_in.at[k], k, 0)

    def square_copy(k):
        return small_copy(square, square_in.at[k], k, 1)

    square[...] = jnp.zeros_like(square)
    for c in range(2):
        load(c, 0).start()
    for c in range(3):
        pack_and_send(c, 0)
        load((c + 2) % 3, (c + 2) // 3).start()
    for k in range(1, group):
        vec_copy(k).start()

    for c in range(3):
        pack_and_send(c, 1)
        load((c + 2) % 3, 1 + (c + 2) // 3).start()

    def tick(u, carry):
        for c in range(3):
            @pl.when(u < chunks)
            def _():
                sum_a(c, u)
        for c in range(3):
            @pl.when((u >= 1) & (u < chunks + 1))
            def _():
                sum_b(c, u - 1)
        for c in range(3):
            @pl.when(u >= 2)
            def _():
                sum_c(c, u - 2)
        for c in range(3):
            @pl.when(u + 2 < chunks)
            def _():
                pack_and_send(c, u + 2)

            nc, nt = (c + 2) % 3, u + 2 + (c + 2) // 3

            @pl.when(nt < chunks)
            def _():
                load(nc, nt).start()
        return carry

    lax.fori_loop(0, chunks + 2, tick, 0)

    vec_sum = gvec[me].astype(F32)
    for k in range(1, group):
        vec_copy(k).wait()
        vec_sum = vec_sum + vec_in[k].astype(F32)
    vec_out[...] = vec_sum
    square[0:1, :] += sum((vec_sum * vec_sum)[:, LANES * k:LANES * (k + 1)] for k in range(vec_sum.shape[1] // LANES))

    for k in range(1, group):
        square_copy(k).start()
    whole = square[...]
    for k in range(1, group):
        square_copy(k).wait_recv()
        whole = whole + square_in[k]
    for k in range(1, group):
        square_copy(k).wait_send()
    norm = jnp.sqrt(jnp.sum(whole, keepdims=True))
    clip_out[...] = jnp.broadcast_to(jnp.minimum(1.0, 1.0 / (norm + NORM_EPS)), clip_out.shape)

    for c in range(3):
        for t in range(chunks - 2, chunks):
            for j in range(3):
                copy_a(c, t, j).wait_send()
            copy_b(c, t).wait_send()
            copy_c(c, t).wait_send()


def reduce_share(grad_mat, grad_vec, group, chunks):
    share_rows = grad_mat.shape[1] // group // LANES
    rows = share_rows // (3 * chunks)
    vec_share = grad_vec.shape[1] // group
    grad = grad_mat.reshape(group, 3, chunks, 1, rows * LANES)
    gvec = grad_vec.reshape(group, 1, vec_share)
    vmem = pl.BlockSpec(memory_space=pltpu.VMEM)
    dma = pltpu.SemaphoreType.DMA
    total, vec, clip = pl.pallas_call(
        functools.partial(reduce_kernel, chunks, rows),
        out_shape=(jax.ShapeDtypeStruct((share_rows, LANES), F32),
                   jax.ShapeDtypeStruct((1, vec_share), F32),
                   jax.ShapeDtypeStruct((8, LANES), F32)),
        in_specs=[pl.BlockSpec(memory_space=pl.ANY), vmem],
        out_specs=(vmem, vmem, vmem),
        scratch_shapes=[
            pltpu.VMEM((2, group, 1, rows * LANES), BF16),
            pltpu.VMEM((3, 2, 4, 4, rows, LANES), BF16),
            pltpu.VMEM((3, SLOTS, 3, 4, rows, LANES), BF16),
            pltpu.VMEM((3, 2, 2, rows, LANES), F32),
            pltpu.VMEM((3, 2, 2, rows, LANES), F32),
            pltpu.VMEM((3, chunks, 2, rows, LANES), F32),
            pltpu.VMEM((3, 2, rows, LANES), F32),
            pltpu.VMEM((3, 2, rows, LANES), F32),
            pltpu.VMEM((3, chunks, rows, LANES), F32),
            pltpu.VMEM((group, 1, vec_share), BF16),
            pltpu.VMEM((8, LANES), F32),
            pltpu.VMEM((group, 8, LANES), F32),
            dma((2,)),
            dma((3, 2, 3)), dma((3, SLOTS, 3)),
            dma((3, 2)), dma((3, chunks)),
            dma((3, 2)), dma((3, chunks)),
            dma((2, group)), dma((2, group)),
            pltpu.SemaphoreType.REGULAR((3, 3)),
        ],
        compiler_params=pltpu.CompilerParams(collective_id=0, has_side_effects=True, vmem_limit_bytes=60 * 1024 * 1024),
        name='reduce_share',
    )(grad, gvec)
    return total.reshape(-1), vec.reshape(-1), clip[0, 0]


def gather_kernel(chunks, rows, share, vec, out, vec_out, send_sem, recv_sem, vec_send, vec_recv, vec_local):
    me = lax.axis_index('fsdp')
    group = 16

    barrier = pltpu.get_barrier_semaphore()
    for k in range(1, group):
        pl.semaphore_signal(barrier, inc=1, device_id=(lax.rem(me + k, group),), device_id_type=MESH)
    pl.semaphore_wait(barrier, group - 1)

    def flip(index, strides):
        for stride in strides:
            index = across(index, stride)
        return index

    def message(c, k, origin, step, sem):
        source = flip(me, origin)
        src = share.at[c, k] if not origin else out.at[source, c, k]
        mask = sum(origin) + step
        return pltpu.make_async_remote_copy(
            src_ref=src, dst_ref=out.at[source, c, k],
            send_sem=send_sem, recv_sem=recv_sem.at[c, k, mask],
            device_id=(across(me, step),), device_id_type=MESH)

    def arrived(c, k, origin):
        pltpu.make_async_remote_copy(
            src_ref=out.at[me, c, k], dst_ref=out.at[flip(me, origin), c, k],
            send_sem=send_sem, recv_sem=recv_sem.at[c, k, sum(origin)],
            device_id=(across(me, 1),), device_id_type=MESH).wait_recv()

    def forward(c, k, origin, steps):
        if origin:
            arrived(c, k, origin)
        for step in steps:
            message(c, k, origin, step, send_sem).start()

    dims = [tuple(STEPS[(c + j) % 3] for j in range(3)) for c in range(3)]

    def vec_copy(k):
        return pltpu.make_async_remote_copy(
            src_ref=vec, dst_ref=vec_out.at[me], send_sem=vec_send.at[k], recv_sem=vec_recv.at[k],
            device_id=(lax.rem(me + k, group),), device_id_type=MESH)

    for which in range(3):
        for c in range(3):
            for k in range(chunks):
                forward(c, k, (), (dims[c][which],))
    for c in range(3):
        for k in range(chunks):
            forward(c, k, (), (1,))
    for k in range(1, group):
        vec_copy(k).start()
    out[me] = share[...]
    vec_out[me] = vec[...]
    for c in range(3):
        d1, d2, d3 = dims[c]
        for k in range(chunks):
            forward(c, k, (d1,), (d2, d3, 1))
    for c in range(3):
        d1, d2, d3 = dims[c]
        for k in range(chunks):
            forward(c, k, (d2,), (d3, 1))
    for c in range(3):
        d1, d2, d3 = dims[c]
        for k in range(chunks):
            forward(c, k, (d3,), (1,))
    for c in range(3):
        d1, d2, d3 = dims[c]
        for k in range(chunks):
            forward(c, k, (d1, d2), (d3, 1))
    for origin in ((0, 2), (1, 2), (0, 1, 2)):
        for c in range(3):
            for k in range(chunks):
                forward(c, k, tuple(dims[c][j] for j in origin), (1,))
    for mask in range(8):
        for c in range(3):
            for k in range(chunks):
                arrived(c, k, tuple(STEPS[j] for j in range(3) if mask // 2 ** j % 2) + (1,))
    for k in range(1, group):
        pltpu.make_async_remote_copy(
            src_ref=vec, dst_ref=vec_out.at[lax.rem(me + group - k, group)], send_sem=vec_send.at[k],
            recv_sem=vec_recv.at[k], device_id=(lax.rem(me + k, group),), device_id_type=MESH).wait()
    pltpu.make_async_copy(out.at[pl.ds(0, group - 1)], out.at[pl.ds(0, group - 1)], send_sem).wait()


def drain_kernel(parts, held, out, sem):
    size = held.shape[0] // parts
    copies = [pltpu.make_async_copy(held.at[pl.ds(k * size, size)], out.at[pl.ds(k * size, size)], sem.at[k])
              for k in range(parts)]
    for copy in copies:
        copy.start()
    for copy in copies:
        copy.wait()


def gather_share(share, vec, group, chunks):
    rows = share.shape[0] // LANES // (3 * chunks)
    vmem = pl.BlockSpec(memory_space=pltpu.VMEM)
    dma = pltpu.SemaphoreType.DMA
    weights, vec_weights = pl.pallas_call(
        functools.partial(gather_kernel, chunks, rows),
        out_shape=(pltpu.VMEM((group, 3, chunks, rows, LANES), BF16),
                   jax.ShapeDtypeStruct((group, 1, vec.shape[0]), BF16)),
        in_specs=[vmem, vmem],
        out_specs=(vmem, vmem),
        scratch_shapes=[dma, dma((3, chunks, 16)), dma((group,)), dma((group,)), dma],
        compiler_params=pltpu.CompilerParams(collective_id=1, has_side_effects=True, vmem_limit_bytes=8 * 1024 * 1024),
        name='gather_share',
    )(share.reshape(3, chunks, rows, LANES), vec.reshape(1, -1))
    weights = pl.pallas_call(
        functools.partial(drain_kernel, 8),
        out_shape=jax.ShapeDtypeStruct(weights.shape, BF16),
        in_specs=[vmem],
        out_specs=pl.BlockSpec(memory_space=pl.ANY),
        scratch_shapes=[dma((8,))],
        compiler_params=pltpu.CompilerParams(vmem_limit_bytes=8 * 1024 * 1024),
        name='drain',
    )(weights)
    return weights.reshape(-1), vec_weights.reshape(-1)


def solution(mesh):
    group = mesh.shape['fsdp']

    def local_step(grad_mat, grad_vec, master_mat, moment_mat, second_mat, master_vec, moment_vec, second_vec):
        sum_mat, sum_vec, clip_coef = reduce_share(grad_mat, grad_vec, group, 12)
        new_mat = adam_update(sum_mat, clip_coef, master_mat, moment_mat, second_mat, DECAY)
        new_vec = adam_update(sum_vec, clip_coef, master_vec, moment_vec, second_vec, 0.0)
        weights_mat, weights_vec = gather_share(new_mat[0].astype(BF16), new_vec[0].astype(BF16), group, 2)
        return new_mat + new_vec + (weights_mat, weights_vec)

    row_spec = P('fsdp', None)
    flat_spec = P('fsdp')
    whole_spec = P()
    return jax.shard_map(local_step, mesh=mesh,
                         in_specs=(row_spec, row_spec) + (flat_spec,) * 6,
                         out_specs=(flat_spec,) * 6 + (whole_spec, whole_spec),
                         check_vma=False)
```

```python
import functools

import jax
import jax.numpy as jnp
from jax import lax
from jax.experimental import pallas as pl
from jax.experimental.pallas import tpu as pltpu
from jax.sharding import PartitionSpec as P

STEP = 4
LEARN_RATE = 1e-3
BETA_ONE = 0.9
BETA_TWO = 0.999
ADAM_EPS = 1e-8
DECAY = 0.01
NORM_EPS = 1e-6
FIX_ONE = 1.0 - BETA_ONE ** STEP
FIX_TWO = 1.0 - BETA_TWO ** STEP

MESH = pl.DeviceIdType.MESH
LANES = 128
SLOTS = 3
STEPS = (2, 4, 8)
F32 = jnp.float32
BF16 = jnp.bfloat16


def adam_update(grad_sum, clip_coef, master, moment, second, decay):
    clip_grad = clip_coef * grad_sum
    new_moment = BETA_ONE * moment + (1.0 - BETA_ONE) * clip_grad
    new_second = BETA_TWO * second + (1.0 - BETA_TWO) * clip_grad * clip_grad
    step_dir = (new_moment / FIX_ONE) / (jnp.sqrt(new_second / FIX_TWO) + ADAM_EPS)
    new_master = master - LEARN_RATE * (step_dir + decay * master)
    return new_master, new_moment, new_second


def bit_of(index, stride):
    return lax.rem(lax.div(index, stride), 2)


def across(index, stride):
    return index + stride * (1 - 2 * bit_of(index, stride))


def reduce_kernel(chunks, rows, grad, gvec, total_out, vec_out, clip_out,
                  raw, packed, recv_a, send_b, keep_b, recv_b, send_c, keep_c, recv_c,
                  vec_in, square, square_in,
                  raw_sem, send_a_sem, recv_a_sem, send_b_sem, recv_b_sem, send_c_sem, recv_c_sem,
                  small_send, small_recv, free_sem):
    me = lax.axis_index('fsdp')
    core = bit_of(me, 1)
    group = 16

    barrier = pltpu.get_barrier_semaphore()
    for k in range(1, group):
        pl.semaphore_signal(barrier, inc=1, device_id=(lax.rem(me + k, group),), device_id_type=MESH)
    pl.semaphore_wait(barrier, group - 1)

    dims = [tuple(STEPS[(c + k) % 3] for k in range(3)) for c in range(3)]

    def load(c, t):
        slot = lax.rem(t + c, 2)
        return pltpu.make_async_copy(grad.at[:, c, t], raw.at[slot], raw_sem.at[slot])

    def peers(c):
        d1 = dims[c][0]
        other = across(me, d1)
        return ((across(me, 1), bit_of(me, d1), 1 - core),
                (other, 1 - bit_of(me, d1), core),
                (across(other, 1), 1 - bit_of(me, d1), 1 - core))

    def copy_a(c, t, j):
        device, d1_bit, core_bit = peers(c)[j]
        ps, rs = lax.rem(t, 2), lax.rem(t, SLOTS)
        return pltpu.make_async_remote_copy(
            src_ref=packed.at[c, ps, 2 * d1_bit + core_bit], dst_ref=recv_a.at[c, rs, j],
            send_sem=send_a_sem.at[c, ps, j], recv_sem=recv_a_sem.at[c, rs, j],
            device_id=(device,), device_id_type=MESH)

    def copy_b(c, t):
        s = lax.rem(t, 2)
        return pltpu.make_async_remote_copy(
            src_ref=send_b.at[c, s], dst_ref=recv_b.at[c, t],
            send_sem=send_b_sem.at[c, s], recv_sem=recv_b_sem.at[c, t],
            device_id=(across(me, dims[c][1]),), device_id_type=MESH)

    def copy_c(c, t):
        s = lax.rem(t, 2)
        return pltpu.make_async_remote_copy(
            src_ref=send_c.at[c, s], dst_ref=recv_c.at[c, t],
            send_sem=send_c_sem.at[c, s], recv_sem=recv_c_sem.at[c, t],
            device_id=(across(me, dims[c][2]),), device_id_type=MESH)

    blk = 96
    blocks = rows // blk

    def pack_and_send(c, t):
        load(c, t).wait()
        ps = lax.rem(t, 2)
        rs = lax.rem(t + c, 2)

        @pl.when(t >= 2)
        def _():
            for j in range(3):
                copy_a(c, t - 2, j).wait_send()

        d1, d2, d3 = dims[c]
        for share in range(group):
            bits = [(share // d) % 2 for d in (d1, 1, d2, d3)]
            quarter, part = 2 * bits[0] + bits[1], 2 * bits[2] + bits[3]

            def body(b, carry):
                start = pl.multiple_of(b * blk, blk)
                flat = raw[rs, share, :, pl.ds(pl.multiple_of(b * blk * LANES, blk * LANES), blk * LANES)]
                packed[c, ps, quarter, part, pl.ds(start, blk), :] = flat.reshape(blk, LANES)
                return carry

            lax.fori_loop(0, blocks, body, 0)

        @pl.when(t >= SLOTS)
        def _():
            for j in range(3):
                pl.semaphore_wait(free_sem.at[c, j], 1)

        for j in range(3):
            copy_a(c, t, j).start()

    def sum_a(c, t):
        ps, rs = lax.rem(t, 2), lax.rem(t, SLOTS)
        d1, d2, d3 = dims[c]
        mine = 2 * bit_of(me, d1) + core
        for j in range(3):
            copy_a(c, t, j).wait_recv()

        @pl.when(t >= 2)
        def _():
            copy_b(c, t - 2).wait_send()

        s = lax.rem(t, 2)
        for target, half in ((send_b, 1 - bit_of(me, d2)), (keep_b, bit_of(me, d2))):
            for k in range(2):
                part = 2 * half + k

                def body(b, carry):
                    here = pl.ds(pl.multiple_of(b * blk, blk), blk)
                    one = packed[c, ps, mine, part, here, :].astype(F32)
                    two = recv_a[c, rs, 0, part, here, :].astype(F32)
                    three = recv_a[c, rs, 1, part, here, :].astype(F32)
                    four = recv_a[c, rs, 2, part, here, :].astype(F32)
                    target[c, s, k, here, :] = (one + two) + (three + four)
                    return carry

                lax.fori_loop(0, blocks, body, 0)
            if target is send_b:
                copy_b(c, t).start()

        @pl.when(t + SLOTS < chunks)
        def _():
            for j in range(3):
                pl.semaphore_signal(free_sem.at[c, j], inc=1, device_id=(peers(c)[j][0],), device_id_type=MESH)

    def sum_b(c, t):
        d3 = dims[c][2]
        copy_b(c, t).wait_recv()

        @pl.when(t >= 2)
        def _():
            copy_c(c, t - 2).wait_send()

        s = lax.rem(t, 2)
        for target, k in ((send_c, 1 - bit_of(me, d3)), (keep_c, bit_of(me, d3))):
            def body(b, carry):
                here = pl.ds(pl.multiple_of(b * blk, blk), blk)
                target[c, s, here, :] = keep_b[c, s, k, here, :] + recv_b[c, t, k, here, :]
                return carry

            lax.fori_loop(0, blocks, body, 0)
            if target is send_c:
                copy_c(c, t).start()

    def sum_c(c, t):
        copy_c(c, t).wait_recv()
        s = lax.rem(t, 2)

        def body(b, running):
            here = pl.ds(pl.multiple_of(b * blk, blk), blk)
            there = pl.ds(pl.multiple_of((c * chunks + t) * rows + b * blk, blk), blk)
            total = keep_c[c, s, here, :] + recv_c[c, t, here, :]
            total_out[there, :] = total
            return running + jnp.sum((total * total).reshape(blk // 8, 8, LANES), axis=0)

        square[...] += lax.fori_loop(0, blocks, body, jnp.zeros((8, LANES), F32))

    def small_copy(src, dst, k, sem):
        return pltpu.make_async_remote_copy(
            src_ref=src, dst_ref=dst, send_sem=small_send.at[sem, k], recv_sem=small_recv.at[sem, k],
            device_id=(lax.rem(me + k, group),), device_id_type=MESH)

    def vec_copy(k):
        return small_copy(gvec.at[lax.rem(me + k, group)], vec_in.at[k], k, 0)

    def square_copy(k):
        return small_copy(square, square_in.at[k], k, 1)

    square[...] = jnp.zeros_like(square)
    for c in range(2):
        load(c, 0).start()
    for c in range(3):
        pack_and_send(c, 0)
        load((c + 2) % 3, (c + 2) // 3).start()
    for k in range(1, group):
        vec_copy(k).start()

    for c in range(3):
        pack_and_send(c, 1)
        load((c + 2) % 3, 1 + (c + 2) // 3).start()

    def tick(u, carry):
        for c in range(3):
            @pl.when(u < chunks)
            def _():
                sum_a(c, u)
        for c in range(3):
            @pl.when((u >= 1) & (u < chunks + 1))
            def _():
                sum_b(c, u - 1)
        for c in range(3):
            @pl.when(u >= 2)
            def _():
                sum_c(c, u - 2)
        for c in range(3):
            @pl.when(u + 2 < chunks)
            def _():
                pack_and_send(c, u + 2)

            nc, nt = (c + 2) % 3, u + 2 + (c + 2) // 3

            @pl.when(nt < chunks)
            def _():
                load(nc, nt).start()
        return carry

    lax.fori_loop(0, chunks + 2, tick, 0)

    vec_sum = gvec[me].astype(F32)
    for k in range(1, group):
        vec_copy(k).wait()
        vec_sum = vec_sum + vec_in[k].astype(F32)
    vec_out[...] = vec_sum
    square[0:1, :] += sum((vec_sum * vec_sum)[:, LANES * k:LANES * (k + 1)] for k in range(vec_sum.shape[1] // LANES))

    for k in range(1, group):
        square_copy(k).start()
    whole = square[...]
    for k in range(1, group):
        square_copy(k).wait_recv()
        whole = whole + square_in[k]
    for k in range(1, group):
        square_copy(k).wait_send()
    norm = jnp.sqrt(jnp.sum(whole, keepdims=True))
    clip_out[...] = jnp.broadcast_to(jnp.minimum(1.0, 1.0 / (norm + NORM_EPS)), clip_out.shape)

    for c in range(3):
        for t in range(chunks - 2, chunks):
            for j in range(3):
                copy_a(c, t, j).wait_send()
            copy_b(c, t).wait_send()
            copy_c(c, t).wait_send()


def reduce_share(grad_mat, grad_vec, group, chunks):
    share_rows = grad_mat.shape[1] // group // LANES
    rows = share_rows // (3 * chunks)
    vec_share = grad_vec.shape[1] // group
    grad = grad_mat.reshape(group, 3, chunks, 1, rows * LANES)
    gvec = grad_vec.reshape(group, 1, vec_share)
    vmem = pl.BlockSpec(memory_space=pltpu.VMEM)
    dma = pltpu.SemaphoreType.DMA
    total, vec, clip = pl.pallas_call(
        functools.partial(reduce_kernel, chunks, rows),
        out_shape=(jax.ShapeDtypeStruct((share_rows, LANES), F32),
                   jax.ShapeDtypeStruct((1, vec_share), F32),
                   jax.ShapeDtypeStruct((8, LANES), F32)),
        in_specs=[pl.BlockSpec(memory_space=pl.ANY), vmem],
        out_specs=(vmem, vmem, vmem),
        scratch_shapes=[
            pltpu.VMEM((2, group, 1, rows * LANES), BF16),
            pltpu.VMEM((3, 2, 4, 4, rows, LANES), BF16),
            pltpu.VMEM((3, SLOTS, 3, 4, rows, LANES), BF16),
            pltpu.VMEM((3, 2, 2, rows, LANES), F32),
            pltpu.VMEM((3, 2, 2, rows, LANES), F32),
            pltpu.VMEM((3, chunks, 2, rows, LANES), F32),
            pltpu.VMEM((3, 2, rows, LANES), F32),
            pltpu.VMEM((3, 2, rows, LANES), F32),
            pltpu.VMEM((3, chunks, rows, LANES), F32),
            pltpu.VMEM((group, 1, vec_share), BF16),
            pltpu.VMEM((8, LANES), F32),
            pltpu.VMEM((group, 8, LANES), F32),
            dma((2,)),
            dma((3, 2, 3)), dma((3, SLOTS, 3)),
            dma((3, 2)), dma((3, chunks)),
            dma((3, 2)), dma((3, chunks)),
            dma((2, group)), dma((2, group)),
            pltpu.SemaphoreType.REGULAR((3, 3)),
        ],
        compiler_params=pltpu.CompilerParams(collective_id=0, has_side_effects=True, vmem_limit_bytes=60 * 1024 * 1024),
        name='reduce_share',
    )(grad, gvec)
    return total, vec, clip


def gather_kernel(chunks, rows, grad, clip, master, moment, second, vec_grad, vec_master, vec_moment, vec_second,
                  out, new_master, new_moment, new_second, vec_out, new_vec_master, new_vec_moment, new_vec_second,
                  grad_buf, vec_share, send_sem, recv_sem, load_sem, vec_send, vec_recv):
    me = lax.axis_index('fsdp')
    group = 16

    def state_loads(c, k):
        return [pltpu.make_async_copy(src.at[c, k], dst.at[c, k], load_sem.at[c, k, j])
                for j, (src, dst) in enumerate(((master, new_master), (moment, new_moment), (second, new_second)))]

    def grad_load(c, k):
        return pltpu.make_async_copy(grad.at[c, k], grad_buf.at[(k * 3 + c) % 2], load_sem.at[c, k, 3])

    order = [(c, k) for k in range(chunks) for c in range(3)]
    for n, (c, k) in enumerate(order):
        if n < 2:
            grad_load(c, k).start()
        for load in state_loads(c, k):
            load.start()

    barrier = pltpu.get_barrier_semaphore()
    for k in range(1, group):
        pl.semaphore_signal(barrier, inc=1, device_id=(lax.rem(me + k, group),), device_id_type=MESH)

    def flip(index, strides):
        for stride in strides:
            index = across(index, stride)
        return index

    def message(c, k, origin, step):
        source = flip(me, origin)
        return pltpu.make_async_remote_copy(
            src_ref=out.at[source, c, k], dst_ref=out.at[source, c, k],
            send_sem=send_sem, recv_sem=recv_sem.at[c, k, sum(origin) + step],
            device_id=(across(me, step),), device_id_type=MESH)

    def arrived(c, k, origin):
        pltpu.make_async_remote_copy(
            src_ref=out.at[me, c, k], dst_ref=out.at[flip(me, origin), c, k],
            send_sem=send_sem, recv_sem=recv_sem.at[c, k, sum(origin)],
            device_id=(across(me, 1),), device_id_type=MESH).wait_recv()

    def forward(c, k, origin, steps):
        arrived(c, k, origin)
        for step in steps:
            message(c, k, origin, step).start()

    dims = [tuple(STEPS[(c + j) % 3] for j in range(3)) for c in range(3)]
    clip_coef = clip[0:1, :]
    blk = 48

    def update(c, k, slot):
        def body(b, carry):
            here = pl.ds(pl.multiple_of(b * blk, blk), blk)
            p, m, v = adam_update(grad_buf[slot, here, :], clip_coef, new_master[c, k, here, :],
                                  new_moment[c, k, here, :], new_second[c, k, here, :], DECAY)
            new_master[c, k, here, :] = p
            new_moment[c, k, here, :] = m
            new_second[c, k, here, :] = v
            out[me, c, k, here, :] = p.astype(BF16)
            return carry

        lax.fori_loop(0, rows // blk, body, 0)

    for n, (c, k) in enumerate(order):
        grad_load(c, k).wait()
        for load in state_loads(c, k):
            load.wait()
        update(c, k, n % 2)
        if n + 2 < len(order):
            grad_load(*order[n + 2]).start()
        if n == 0:
            pl.semaphore_wait(barrier, group - 1)
        for step in dims[c] + (1,):
            message(c, k, (), step).start()

    def vec_copy(k):
        return pltpu.make_async_remote_copy(
            src_ref=vec_share, dst_ref=vec_out.at[me], send_sem=vec_send.at[k], recv_sem=vec_recv.at[k],
            device_id=(lax.rem(me + k, group),), device_id_type=MESH)

    width = vec_share.shape[1]
    p, m, v = adam_update(vec_grad[...], clip[0:1, 0:1], vec_master[...].reshape(1, width), vec_moment[...].reshape(1, width),
                          vec_second[...].reshape(1, width), 0.0)
    new_vec_master[...] = p
    new_vec_moment[...] = m
    new_vec_second[...] = v
    vec_share[...] = p.astype(BF16)
    vec_out[me] = p.astype(BF16)
    for k in range(1, group):
        vec_copy(k).start()

    for c in range(3):
        d1, d2, d3 = dims[c]
        for k in range(chunks):
            forward(c, k, (d1,), (d2, d3, 1))
    for c in range(3):
        d1, d2, d3 = dims[c]
        for k in range(chunks):
            forward(c, k, (d2,), (d3, 1))
    for c in range(3):
        d1, d2, d3 = dims[c]
        for k in range(chunks):
            forward(c, k, (d3,), (1,))
    for c in range(3):
        d1, d2, d3 = dims[c]
        for k in range(chunks):
            forward(c, k, (d1, d2), (d3, 1))
    for origin in ((0, 2), (1, 2), (0, 1, 2)):
        for c in range(3):
            for k in range(chunks):
                forward(c, k, tuple(dims[c][j] for j in origin), (1,))
    for mask in range(8):
        for c in range(3):
            for k in range(chunks):
                arrived(c, k, tuple(STEPS[j] for j in range(3) if mask // 2 ** j % 2) + (1,))
    for k in range(1, group):
        pltpu.make_async_remote_copy(
            src_ref=vec_share, dst_ref=vec_out.at[lax.rem(me + group - k, group)], send_sem=vec_send.at[k],
            recv_sem=vec_recv.at[k], device_id=(lax.rem(me + k, group),), device_id_type=MESH).wait()
    pltpu.make_async_copy(out.at[pl.ds(0, group - 1)], out.at[pl.ds(0, group - 1)], send_sem).wait()


def drain_kernel(parts, *refs):
    held, out, sem = refs[:4], refs[5:9], refs[-1]
    copies = []
    for j in range(4):
        pieces = parts if j == 0 else 1
        size = held[j].shape[0] // pieces
        copies += [pltpu.make_async_copy(held[j].at[pl.ds(k * size, size)], out[j].at[pl.ds(k * size, size)],
                                         sem.at[len(copies) + k]) for k in range(pieces)]
    for copy in copies:
        copy.start()
    vec, vec_out = refs[4], refs[9]
    vec_out[...] = jnp.concatenate([vec[k].astype(F32).reshape(-1, LANES) for k in range(vec.shape[0])], axis=0).astype(BF16)
    for copy in copies:
        copy.wait()


def update_and_gather(total, clip, state, vec_grad, vec_state, group, chunks):
    rows = total.shape[0] // (3 * chunks)
    width = vec_grad.shape[1]
    shape = (3, chunks, rows, LANES)
    vmem, anywhere = pl.BlockSpec(memory_space=pltpu.VMEM), pl.BlockSpec(memory_space=pl.ANY)
    dma = pltpu.SemaphoreType.DMA
    vec_shape = jax.ShapeDtypeStruct((1, width), F32)
    results = pl.pallas_call(
        functools.partial(gather_kernel, chunks, rows),
        out_shape=(pltpu.VMEM((group,) + shape, BF16),) + (pltpu.VMEM(shape, F32),) * 3
        + (jax.ShapeDtypeStruct((group, 1, width), BF16),) + (vec_shape,) * 3,
        in_specs=[anywhere, vmem] + [anywhere] * 3 + [vmem] * 4,
        out_specs=(vmem,) * 8,
        scratch_shapes=[pltpu.VMEM((2, rows, LANES), F32), pltpu.VMEM((1, width), BF16),
                        dma, dma((3, chunks, 16)), dma((3, chunks, 4)), dma((group,)), dma((group,))],
        compiler_params=pltpu.CompilerParams(collective_id=1, has_side_effects=True, vmem_limit_bytes=4 * 1024 * 1024),
        name='update_gather',
    )(total.reshape(shape), clip, *[x.reshape(shape) for x in state], vec_grad, *vec_state)
    parts = 8
    drained = pl.pallas_call(
        functools.partial(drain_kernel, parts),
        out_shape=tuple(jax.ShapeDtypeStruct(x.shape, x.dtype) for x in results[:4])
        + (jax.ShapeDtypeStruct((group * width // LANES, LANES), BF16),),
        in_specs=[vmem] * 5,
        out_specs=(anywhere,) * 4 + (vmem,),
        scratch_shapes=[dma((parts + 3,))],
        compiler_params=pltpu.CompilerParams(vmem_limit_bytes=4 * 1024 * 1024),
        name='drain',
    )(*[pltpu.with_memory_space_constraint(x, pltpu.VMEM) for x in results[:4]], results[4])
    flat = [x.reshape(-1) for x in drained]
    return tuple(flat[1:4]) + tuple(x.reshape(-1) for x in results[5:8]) + (flat[0], flat[4])


def solution(mesh):
    group = mesh.shape['fsdp']

    def local_step(grad_mat, grad_vec, master_mat, moment_mat, second_mat, master_vec, moment_vec, second_vec):
        total, vec_grad, clip = reduce_share(grad_mat, grad_vec, group, 12)
        return update_and_gather(total, clip, (master_mat, moment_mat, second_mat), vec_grad,
                                 (master_vec, moment_vec, second_vec), group, 4)

    row_spec = P('fsdp', None)
    flat_spec = P('fsdp')
    whole_spec = P()
    return jax.shard_map(local_step, mesh=mesh,
                         in_specs=(row_spec, row_spec) + (flat_spec,) * 6,
                         out_specs=(flat_spec,) * 6 + (whole_spec, whole_spec),
                         check_vma=False)
```

```python
import functools

import jax
import jax.numpy as jnp
from jax import lax
from jax.experimental import pallas as pl
from jax.experimental.pallas import tpu as pltpu
from jax.sharding import PartitionSpec as P

STEP = 4
LEARN_RATE = 1e-3
BETA_ONE = 0.9
BETA_TWO = 0.999
ADAM_EPS = 1e-8
DECAY = 0.01
NORM_EPS = 1e-6
FIX_ONE = 1.0 - BETA_ONE ** STEP
FIX_TWO = 1.0 - BETA_TWO ** STEP

MESH = pl.DeviceIdType.MESH
LANES = 128
GROUP = 16
STRIDES = (2, 4, 8)
DIMS = tuple(tuple(STRIDES[(c + j) % 3] for j in range(3)) for c in range(3))
PACK_SLOTS = 3
F32 = jnp.float32
BF16 = jnp.bfloat16


def adam_update(grad_sum, clip_coef, master, moment, second, decay):
    clip_grad = clip_coef * grad_sum
    new_moment = BETA_ONE * moment + (1.0 - BETA_ONE) * clip_grad
    new_second = BETA_TWO * second + (1.0 - BETA_TWO) * clip_grad * clip_grad
    step_dir = (new_moment / FIX_ONE) / (jnp.sqrt(new_second / FIX_TWO) + ADAM_EPS)
    new_master = master - LEARN_RATE * (step_dir + decay * master)
    return new_master, new_moment, new_second


def bit_of(index, stride):
    return lax.rem(lax.div(index, stride), 2)


def across(index, stride):
    return index + stride * (1 - 2 * bit_of(index, stride))


def flip(index, strides):
    for stride in strides:
        index = across(index, stride)
    return index


def aligned(start, size):
    return pl.ds(pl.multiple_of(start, 16), size)


def step_kernel(chunks, rows, parts, grad, gvec, master, moment, second, vec_master, vec_moment, vec_second,
                out, state, vec_out, vec_state,
                raw, send_b, keep_b, stage, vec_in, vec_total, vec_share, square, square_in,
                raw_sem, send_a_sem, recv_a_sem, send_b_sem, recv_b_sem, send_c_sem, recv_c_sem,
                vec_send, vec_recv, square_send, square_recv, stage_sem, state_sem,
                send_sem, recv_sem, share_send, share_recv):
    me = lax.axis_index('fsdp')
    core = bit_of(me, 1)
    share_rows = 3 * chunks * rows
    span = share_rows // (3 * parts)

    def packed(c, t, quarter):
        return aligned(((c * PACK_SLOTS + lax.rem(t, PACK_SLOTS)) * 4 + quarter) * 4 * rows, 4 * rows)

    def landed(c, t, j):
        return aligned((3 * PACK_SLOTS * 4 + (c * chunks + t) * 3 + j) * 4 * rows, 4 * rows)

    def half_sums(c, t):
        return aligned(share_rows + (c * chunks + t) * 2 * rows, 2 * rows)

    def totals(c, t):
        return aligned((c * chunks + t) * rows, rows)

    def load(c, t):
        slot = lax.rem(t + c, 2)
        return pltpu.make_async_copy(grad.at[:, c, t], raw.at[slot], raw_sem.at[slot])

    def copy_a(c, t, j):
        d1 = DIMS[c][0]
        mine, other = bit_of(me, d1), across(me, d1)
        device, d1_bit, core_bit = ((across(me, 1), mine, 1 - core), (other, 1 - mine, core),
                                    (across(other, 1), 1 - mine, 1 - core))[j]
        return pltpu.make_async_remote_copy(
            src_ref=out.at[packed(c, t, 2 * d1_bit + core_bit)], dst_ref=out.at[landed(c, t, j)],
            send_sem=send_a_sem.at[c, lax.rem(t, PACK_SLOTS), j], recv_sem=recv_a_sem.at[c, t, j],
            device_id=(device,), device_id_type=MESH)

    def copy_b(c, t):
        s = lax.rem(t, 2)
        return pltpu.make_async_remote_copy(
            src_ref=send_b.at[c, s], dst_ref=state.at[half_sums(c, t)],
            send_sem=send_b_sem.at[c, s], recv_sem=recv_b_sem.at[c, t],
            device_id=(across(me, DIMS[c][1]),), device_id_type=MESH)

    def copy_c(c, t):
        away = 1 - bit_of(me, DIMS[c][2])
        source = aligned(share_rows + ((c * chunks + t) * 2 + away) * rows, rows)
        return pltpu.make_async_remote_copy(
            src_ref=state.at[source], dst_ref=state.at[totals(c, t)],
            send_sem=send_c_sem, recv_sem=recv_c_sem.at[c, t],
            device_id=(across(me, DIMS[c][2]),), device_id_type=MESH)

    blk = 96
    blocks = rows // blk

    def pack(c, t):
        load(c, t).wait()
        slot = lax.rem(t + c, 2)

        @pl.when(t >= PACK_SLOTS)
        def _():
            for j in range(3):
                copy_a(c, t - PACK_SLOTS, j).wait_send()

        base = (c * PACK_SLOTS + lax.rem(t, PACK_SLOTS)) * 16 * rows
        for share in range(GROUP):
            d1_bit, core_bit, d2_bit, d3_bit = [(share // d) % 2 for d in (DIMS[c][0], 1) + DIMS[c][1:]]
            place = 8 * d1_bit + 4 * core_bit + 2 * d2_bit + d3_bit

            def body(b, carry):
                columns = pl.ds(pl.multiple_of(b * blk * LANES, blk * LANES), blk * LANES)
                out[aligned(base + place * rows + b * blk, blk), :] = raw[slot, share, :, columns].reshape(blk, LANES)
                return carry

            lax.fori_loop(0, blocks, body, 0)

    def send_a(c, t):
        for j in range(3):
            copy_a(c, t, j).start()

    def load_after(c, t):
        nc, nt = (c + 2) % 3, t + (c + 2) // 3

        @pl.when(nt < chunks)
        def _():
            load(nc, nt).start()

    def sum_a(c, t):
        d1, d2, d3 = DIMS[c]
        own = ((c * PACK_SLOTS + lax.rem(t, PACK_SLOTS)) * 4 + 2 * bit_of(me, d1) + core) * 4 * rows
        others = [(3 * PACK_SLOTS * 4 + (c * chunks + t) * 3 + j) * 4 * rows for j in range(3)]
        for j in range(3):
            copy_a(c, t, j).wait_recv()

        @pl.when(t >= 2)
        def _():
            copy_b(c, t - 2).wait_send()

        s = lax.rem(t, 2)
        for target, half in ((send_b, 1 - bit_of(me, d2)), (keep_b, bit_of(me, d2))):
            def body(b, carry):
                shift = half * 2 * rows + b * blk
                one, two, three, four = [out[aligned(base + shift, blk), :].astype(F32) for base in [own] + others]
                target[c, s, aligned(b * blk, blk), :] = (one + two) + (three + four)
                return carry

            lax.fori_loop(0, 2 * blocks, body, 0)
            if target is send_b:
                copy_b(c, t).start()

    def sum_b(c, t):
        d3 = DIMS[c][2]
        copy_b(c, t).wait_recv()
        s = lax.rem(t, 2)
        mine = bit_of(me, d3)

        def add(k):
            def body(b, carry):
                held = aligned(share_rows + ((c * chunks + t) * 2 + k) * rows + b * blk, blk)
                state[held, :] = keep_b[c, s, aligned(k * rows + b * blk, blk), :] + state[held, :]
                return carry

            lax.fori_loop(0, blocks, body, 0)

        add(1 - mine)
        copy_c(c, t).start()
        add(mine)

    def sum_c(c, t):
        copy_c(c, t).wait_recv()
        mine = bit_of(me, DIMS[c][2])

        def body(b, running):
            held = aligned(share_rows + ((c * chunks + t) * 2 + mine) * rows + b * blk, blk)
            here = aligned((c * chunks + t) * rows + b * blk, blk)
            total = state[held, :] + state[here, :]
            state[here, :] = total
            return running + jnp.sum((total * total).reshape(blk // 8, 8, LANES), axis=0)

        square[...] += lax.fori_loop(0, blocks, body, jnp.zeros((8, LANES), F32))

    def small_copy(src, dst, k, sends, recvs):
        return pltpu.make_async_remote_copy(
            src_ref=src, dst_ref=dst, send_sem=sends.at[k], recv_sem=recvs.at[k],
            device_id=(lax.rem(me + k, GROUP),), device_id_type=MESH)

    def vec_copy(k):
        return small_copy(gvec.at[lax.rem(me + k, GROUP)], vec_in.at[k], k, vec_send, vec_recv)

    def square_copy(k):
        return small_copy(square, square_in.at[k], k, square_send, square_recv)

    barrier = pltpu.get_barrier_semaphore()
    for k in range(1, GROUP):
        pl.semaphore_signal(barrier, inc=1, device_id=(lax.rem(me + k, GROUP),), device_id_type=MESH)
    for c in range(2):
        load(c, 0).start()
    square[...] = jnp.zeros_like(square)
    pack(0, 0)
    pl.semaphore_wait(barrier, GROUP - 1)
    send_a(0, 0)
    load_after(0, 0)
    for t in range(2):
        for c in range(1 if t == 0 else 0, 3):
            pack(c, t)
            send_a(c, t)
            load_after(c, t)
    for k in range(1, GROUP):
        vec_copy(k).start()

    def tick(u, carry):
        for c in range(3):
            @pl.when(u < chunks)
            def _():
                sum_a(c, u)
        for c in range(3):
            @pl.when((u >= 1) & (u < chunks + 1))
            def _():
                sum_b(c, u - 1)
        for c in range(3):
            @pl.when(u >= 2)
            def _():
                sum_c(c, u - 2)
        for c in range(3):
            @pl.when(u + 2 < chunks)
            def _():
                pack(c, u + 2)
                send_a(c, u + 2)
                load_after(c, u + 2)

        @pl.when(u == chunks // 2)
        def _():
            total = gvec[me].astype(F32)
            for k in range(1, GROUP):
                vec_copy(k).wait()
                total = total + vec_in[k].astype(F32)
            padding = jnp.zeros((1, vec_total.shape[1] - total.shape[1]), F32)
            vec_total[...] = jnp.concatenate([total, padding], axis=1)
            square[0:1, :] += sum((total * total)[:, LANES * k:LANES * (k + 1)] for k in range(total.shape[1] // LANES))

        return carry

    lax.fori_loop(0, chunks + 2, tick, 0)

    for c in range(3):
        for t in range(chunks - PACK_SLOTS, chunks):
            for j in range(3):
                copy_a(c, t, j).wait_send()
    for k in range(1, GROUP):
        square_copy(k).start()

    pltpu.make_async_copy(state.at[pl.ds(0, share_rows)], state.at[pl.ds(0, share_rows)], send_c_sem).wait()
    for c in range(3):
        for t in range(chunks - 2, chunks):
            copy_b(c, t).wait_send()

    order = [(c, k) for k in range(parts) for c in range(3)]

    def place(c, k, which=0):
        return pl.ds(which * share_rows + (c * parts + k) * span, span)

    def master_load(n):
        return pltpu.make_async_copy(master.at[place(*order[n])], stage.at[n % 2], stage_sem.at[n % 2])

    def state_loads(c, k):
        return [pltpu.make_async_copy(src.at[place(c, k)], state.at[place(c, k, 1 + j)], state_sem.at[c, k, j])
                for j, src in enumerate((moment, second))]

    for n, (c, k) in enumerate(order):
        if n < 2:
            master_load(n).start()
        for one in state_loads(c, k):
            one.start()

    whole = square[...]
    for k in range(1, GROUP):
        square_copy(k).wait_recv()
        whole = whole + square_in[k]
    norm = jnp.sqrt(jnp.sum(whole, keepdims=True))
    clip_one = jnp.minimum(1.0, 1.0 / (norm + NORM_EPS))
    clip_coef = jnp.broadcast_to(clip_one, (1, LANES))

    def block(source, c, k):
        return aligned(source * share_rows + (c * parts + k) * span, span)

    def message(c, k, origin, step):
        here = block(flip(me, origin), c, k)
        return pltpu.make_async_remote_copy(
            src_ref=out.at[here], dst_ref=out.at[here],
            send_sem=send_sem, recv_sem=recv_sem.at[c, k, sum(origin) + step],
            device_id=(across(me, step),), device_id_type=MESH)

    def arrived(c, k, origin):
        pltpu.make_async_remote_copy(
            src_ref=out.at[block(me, c, k)], dst_ref=out.at[block(flip(me, origin), c, k)],
            send_sem=send_sem, recv_sem=recv_sem.at[c, k, sum(origin)],
            device_id=(across(me, 1),), device_id_type=MESH).wait_recv()

    def forward(c, k, origin, steps):
        arrived(c, k, origin)
        for step in steps:
            message(c, k, origin, step).start()

    step_blk = 48

    def update(n, c, k):
        def body(b, carry):
            first = (c * parts + k) * span + b * step_blk
            here, there, last = [aligned(first + j * share_rows, step_blk) for j in range(3)]
            p, m, v = adam_update(state[here, :], clip_coef, stage[n % 2, aligned(b * step_blk, step_blk), :],
                                  state[there, :], state[last, :], DECAY)
            state[here, :] = p
            state[there, :] = m
            state[last, :] = v
            out[aligned(me * share_rows + first, step_blk), :] = p.astype(BF16)
            return carry

        lax.fori_loop(0, span // step_blk, body, 0)

    for n, (c, k) in enumerate(order):
        master_load(n).wait()
        for one in state_loads(c, k):
            one.wait()
        update(n, c, k)
        if n + 2 < len(order):
            master_load(n + 2).start()
        for step in DIMS[c] + (1,):
            message(c, k, (), step).start()

    def share_copy(k, source):
        return small_copy(vec_share, vec_out.at[source], k, share_send, share_recv)

    width = vec_share.shape[1]
    old = [x[...].reshape(1, width) for x in (vec_master, vec_moment, vec_second)]
    fresh = adam_update(vec_total[...][:, :width], clip_one, *old, 0.0)
    for j in range(3):
        vec_state[j] = fresh[j]
    vec_share[...] = fresh[0].astype(BF16)
    vec_out[me] = fresh[0].astype(BF16)
    for k in range(1, GROUP):
        share_copy(k, me).start()

    for origin, steps in (((0,), (1, 2)), ((1,), (2,)), ((2,), ()), ((0, 1), (2,)), ((0, 2), ()), ((1, 2), ()), ((0, 1, 2), ())):
        for c in range(3):
            for k in range(parts):
                forward(c, k, tuple(DIMS[c][j] for j in origin), tuple(DIMS[c][j] for j in steps) + (1,))
    for mask in range(8):
        for c in range(3):
            for k in range(parts):
                arrived(c, k, tuple(STRIDES[j] for j in range(3) if mask // 2 ** j % 2) + (1,))
    for k in range(1, GROUP):
        square_copy(k).wait_send()
        share_copy(k, lax.rem(me + GROUP - k, GROUP)).wait()
    sent = pl.ds(0, (GROUP - 1) * share_rows)
    pltpu.make_async_copy(out.at[sent], out.at[sent], send_sem).wait()


def drain_kernel(pieces, weights, state, vec, vec_state, weights_out, master, moment, second,
                 vec_out, vec_master, vec_moment, vec_second, sem):
    copies = []
    share_rows = master.shape[0]
    for src, start, dst, count in ((weights, 0, weights_out, 4 * pieces), (state, 0, master, pieces),
                                   (state, share_rows, moment, pieces), (state, 2 * share_rows, second, pieces)):
        size = dst.shape[0] // count
        copies += [pltpu.make_async_copy(src.at[pl.ds(start + k * size, size)], dst.at[pl.ds(k * size, size)],
                                         sem.at[len(copies) + k]) for k in range(count)]
    copies += [pltpu.make_async_copy(vec_state.at[j, 0], dst, sem.at[len(copies) + j])
               for j, dst in enumerate((vec_master, vec_moment, vec_second))]
    for copy in copies:
        copy.start()
    vec_out[...] = jnp.concatenate([vec[k].astype(F32).reshape(-1, LANES) for k in range(vec.shape[0])], axis=0).astype(BF16)
    for copy in copies:
        copy.wait()


def full_step(grad_mat, grad_vec, state, vec_state, chunks, parts):
    share_rows = grad_mat.shape[1] // GROUP // LANES
    rows = share_rows // (3 * chunks)
    span = share_rows // (3 * parts)
    width = grad_vec.shape[1] // GROUP
    vmem, anywhere = pl.BlockSpec(memory_space=pltpu.VMEM), pl.BlockSpec(memory_space=pl.ANY)
    dma = pltpu.SemaphoreType.DMA
    held = pl.pallas_call(
        functools.partial(step_kernel, chunks, rows, parts),
        out_shape=(pltpu.VMEM((GROUP * share_rows, LANES), BF16), pltpu.VMEM((3 * share_rows, LANES), F32),
                   pltpu.VMEM((GROUP, 1, width), BF16), pltpu.VMEM((3, 1, width), F32)),
        in_specs=[anywhere, vmem] + [anywhere] * 3 + [vmem] * 3,
        out_specs=(vmem,) * 4,
        scratch_shapes=[
            pltpu.VMEM((2, GROUP, 1, rows * LANES), BF16),
            pltpu.VMEM((3, 2, 2 * rows, LANES), F32),
            pltpu.VMEM((3, 2, 2 * rows, LANES), F32),
            pltpu.VMEM((2, span, LANES), F32),
            pltpu.VMEM((GROUP, 1, width), BF16),
            pltpu.VMEM((1, -(-width // 1024) * 1024), F32),
            pltpu.VMEM((1, width), BF16),
            pltpu.VMEM((8, LANES), F32),
            pltpu.VMEM((GROUP, 8, LANES), F32),
            dma((2,)), dma((3, PACK_SLOTS, 3)), dma((3, chunks, 3)), dma((3, 2)), dma((3, chunks)), dma, dma((3, chunks)),
            dma((GROUP,)), dma((GROUP,)), dma((GROUP,)), dma((GROUP,)), dma((2,)), dma((3, parts, 2)),
            dma, dma((3, parts, GROUP)), dma((GROUP,)), dma((GROUP,)),
        ],
        compiler_params=pltpu.CompilerParams(collective_id=0, has_side_effects=True, vmem_limit_bytes=14 * 512 * 1024),
        name='full_step',
    )(grad_mat.reshape(GROUP, 3, chunks, 1, rows * LANES), grad_vec.reshape(GROUP, 1, width),
      *[x.reshape(share_rows, LANES) for x in state], *vec_state)
    pieces = 4
    states = jax.ShapeDtypeStruct((share_rows, LANES), F32)
    vectors = jax.ShapeDtypeStruct((width,), F32)
    weights, *rest = pl.pallas_call(
        functools.partial(drain_kernel, pieces),
        out_shape=(jax.ShapeDtypeStruct((GROUP * share_rows, LANES), BF16), states, states, states,
                   jax.ShapeDtypeStruct((GROUP * width // LANES, LANES), BF16), vectors, vectors, vectors),
        in_specs=[vmem] * 4,
        out_specs=(anywhere,) * 4 + (vmem,) + (anywhere,) * 3,
        scratch_shapes=[dma((7 * pieces + 3,))],
        compiler_params=pltpu.CompilerParams(vmem_limit_bytes=7 * 1024 * 1024),
        name='drain',
    )(*[pltpu.with_memory_space_constraint(x, pltpu.VMEM) for x in held])
    flat = [x.reshape(-1) for x in rest]
    return tuple(flat[:3] + flat[4:] + [weights.reshape(-1), flat[3]])


def solution(mesh):
    def local_step(grad_mat, grad_vec, master_mat, moment_mat, second_mat, master_vec, moment_vec, second_vec):
        return full_step(grad_mat, grad_vec, (master_mat, moment_mat, second_mat),
                         (master_vec, moment_vec, second_vec), 18, 4)

    row_spec = P('fsdp', None)
    flat_spec = P('fsdp')
    whole_spec = P()
    return jax.shard_map(local_step, mesh=mesh,
                         in_specs=(row_spec, row_spec) + (flat_spec,) * 6,
                         out_specs=(flat_spec,) * 6 + (whole_spec, whole_spec),
                         check_vma=False)
```

```python
import functools

import jax
import jax.numpy as jnp
from jax import lax
from jax.experimental import pallas as pl
from jax.experimental.pallas import tpu as pltpu
from jax.sharding import PartitionSpec as P

STEP = 4
LEARN_RATE = 1e-3
BETA_ONE = 0.9
BETA_TWO = 0.999
ADAM_EPS = 1e-8
DECAY = 0.01
NORM_EPS = 1e-6
FIX_ONE = 1.0 - BETA_ONE ** STEP
FIX_TWO = 1.0 - BETA_TWO ** STEP

MESH = pl.DeviceIdType.MESH
LANES = 128
GROUP = 16
STRIDES = (2, 4, 8)
DIMS = tuple(tuple(STRIDES[(c + j) % 3] for j in range(3)) for c in range(3))
PACK_SLOTS = 4
F32 = jnp.float32
BF16 = jnp.bfloat16


def adam_update(grad_sum, clip_coef, master, moment, second, decay):
    clip_grad = clip_coef * grad_sum
    new_moment = BETA_ONE * moment + (1.0 - BETA_ONE) * clip_grad
    new_second = BETA_TWO * second + (1.0 - BETA_TWO) * clip_grad * clip_grad
    step_dir = (new_moment / FIX_ONE) / (jnp.sqrt(new_second / FIX_TWO) + ADAM_EPS)
    new_master = master - LEARN_RATE * (step_dir + decay * master)
    return new_master, new_moment, new_second


def bit_of(index, stride):
    return lax.rem(lax.div(index, stride), 2)


def across(index, stride):
    return index + stride * (1 - 2 * bit_of(index, stride))


def flip(index, strides):
    for stride in strides:
        index = across(index, stride)
    return index


def aligned(start, size):
    return pl.ds(pl.multiple_of(start, 16), size)


def step_kernel(chunks, rows, parts, grad, gvec, master, moment, second, vec_master, vec_moment, vec_second,
                out, state, vec_out, vec_state,
                raw, send_b, stage, vec_in, lines, vec_total, vec_share, square, square_in,
                line_sem, raw_sem, send_a_sem, recv_a_sem, send_b_sem, recv_b_sem, send_c_sem, recv_c_sem,
                vec_send, vec_recv, square_send, square_recv, stage_sem, state_sem,
                send_sem, recv_sem, share_send, share_recv):
    me = lax.axis_index('fsdp')
    core = bit_of(me, 1)
    share_rows = 3 * chunks * rows
    span = share_rows // (3 * parts)

    def packed(c, t, quarter):
        return aligned(((c * PACK_SLOTS + lax.rem(t, PACK_SLOTS)) * 4 + quarter) * 4 * rows, 4 * rows)

    def landed(c, t, j):
        return aligned((3 * PACK_SLOTS * 4 + (c * chunks + t) * 3 + j) * 4 * rows, 4 * rows)

    def half_sums(c, t):
        return aligned(share_rows + (c * chunks + t) * 2 * rows, 2 * rows)

    def totals(c, t):
        return aligned((c * chunks + t) * rows, rows)

    def load(c, t):
        return pltpu.make_async_copy(grad.at[:, c, t], raw.at[c], raw_sem.at[c])

    def copy_a(c, t, j):
        d1 = DIMS[c][0]
        mine, other = bit_of(me, d1), across(me, d1)
        device, d1_bit, core_bit = ((across(me, 1), mine, 1 - core), (other, 1 - mine, core),
                                    (across(other, 1), 1 - mine, 1 - core))[j]
        return pltpu.make_async_remote_copy(
            src_ref=out.at[packed(c, t, 2 * d1_bit + core_bit)], dst_ref=out.at[landed(c, t, j)],
            send_sem=send_a_sem.at[c, lax.rem(t, PACK_SLOTS), j], recv_sem=recv_a_sem.at[c, t, j],
            device_id=(device,), device_id_type=MESH)

    def copy_b(c, t):
        s = lax.rem(t, 2)
        return pltpu.make_async_remote_copy(
            src_ref=send_b.at[c, s], dst_ref=state.at[half_sums(c, t)],
            send_sem=send_b_sem.at[c, s], recv_sem=recv_b_sem.at[c, t],
            device_id=(across(me, DIMS[c][1]),), device_id_type=MESH)

    def copy_c(c, t):
        away = 1 - bit_of(me, DIMS[c][2])
        source = aligned(share_rows + ((c * chunks + t) * 2 + away) * rows, rows)
        return pltpu.make_async_remote_copy(
            src_ref=state.at[source], dst_ref=state.at[totals(c, t)],
            send_sem=send_c_sem, recv_sem=recv_c_sem.at[c, t],
            device_id=(across(me, DIMS[c][2]),), device_id_type=MESH)

    blk = 192
    blocks = rows // blk

    def pack(c, t):
        load(c, t).wait()

        @pl.when(t >= PACK_SLOTS)
        def _():
            for j in range(3):
                copy_a(c, t - PACK_SLOTS, j).wait_send()

        base = (c * PACK_SLOTS + lax.rem(t, PACK_SLOTS)) * 16 * rows
        for share in range(GROUP):
            d1_bit, core_bit, d2_bit, d3_bit = [(share // d) % 2 for d in (DIMS[c][0], 1) + DIMS[c][1:]]
            place = 8 * d1_bit + 4 * core_bit + 2 * d2_bit + d3_bit

            def body(b, carry):
                columns = pl.ds(pl.multiple_of(b * blk * LANES, blk * LANES), blk * LANES)
                out[aligned(base + place * rows + b * blk, blk), :] = raw[c, share, :, columns].reshape(blk, LANES)
                return carry

            lax.fori_loop(0, blocks, body, 0)

    def send_a(c, t):
        for j in range(3):
            copy_a(c, t, j).start()

    def load_after(c, t):
        @pl.when(t + 1 < chunks)
        def _():
            load(c, t + 1).start()

    def local_sum(c, t, row):
        own = ((c * PACK_SLOTS + lax.rem(t, PACK_SLOTS)) * 4 + 2 * bit_of(me, DIMS[c][0]) + core) * 4 * rows
        others = [(3 * PACK_SLOTS * 4 + (c * chunks + t) * 3 + j) * 4 * rows for j in range(3)]
        one, two, three, four = [out[aligned(base + row, blk), :].astype(F32) for base in [own] + others]
        return (one + two) + (three + four)

    def sum_a(c, t):
        for j in range(3):
            copy_a(c, t, j).wait_recv()

        @pl.when(t >= 2)
        def _():
            copy_b(c, t - 2).wait_send()

        away = 1 - bit_of(me, DIMS[c][1])

        def body(b, carry):
            send_b[c, lax.rem(t, 2), aligned(b * blk, blk), :] = local_sum(c, t, away * 2 * rows + b * blk)
            return carry

        lax.fori_loop(0, 2 * blocks, body, 0)
        copy_b(c, t).start()

    def sum_b(c, t):
        copy_b(c, t).wait_recv()
        near, mine = bit_of(me, DIMS[c][1]), bit_of(me, DIMS[c][2])

        def add(k):
            def body(b, carry):
                held = aligned(share_rows + ((c * chunks + t) * 2 + k) * rows + b * blk, blk)
                state[held, :] = local_sum(c, t, (near * 2 + k) * rows + b * blk) + state[held, :]
                return carry

            lax.fori_loop(0, blocks, body, 0)

        add(1 - mine)
        copy_c(c, t).start()
        add(mine)

    def sum_c(c, t):
        copy_c(c, t).wait_recv()
        mine = bit_of(me, DIMS[c][2])

        def body(b, running):
            held = aligned(share_rows + ((c * chunks + t) * 2 + mine) * rows + b * blk, blk)
            here = aligned((c * chunks + t) * rows + b * blk, blk)
            total = state[held, :] + state[here, :]
            state[here, :] = total
            return running + jnp.sum((total * total).reshape(blk // 8, 8, LANES), axis=0)

        square[...] += lax.fori_loop(0, blocks, body, jnp.zeros((8, LANES), F32))

    def small_copy(src, dst, k, sends, recvs):
        return pltpu.make_async_remote_copy(
            src_ref=src, dst_ref=dst, send_sem=sends.at[k], recv_sem=recvs.at[k],
            device_id=(lax.rem(me + k, GROUP),), device_id_type=MESH)

    def vec_copy(k):
        return small_copy(gvec.at[lax.rem(me + k, GROUP)], vec_in.at[k], k, vec_send, vec_recv)

    def square_copy(k):
        return small_copy(square, square_in.at[k], k, square_send, square_recv)

    barrier = pltpu.get_barrier_semaphore()
    for k in range(1, GROUP):
        pl.semaphore_signal(barrier, inc=1, device_id=(lax.rem(me + k, GROUP),), device_id_type=MESH)
    for c in range(3):
        load(c, 0).start()
    square[...] = jnp.zeros_like(square)
    pack(0, 0)
    pl.semaphore_wait(barrier, GROUP - 1)
    send_a(0, 0)
    load_after(0, 0)
    for t in range(2):
        for c in range(1 if t == 0 else 0, 3):
            pack(c, t)
            send_a(c, t)
            load_after(c, t)
    own_vec = pltpu.make_async_copy(gvec.at[me], vec_in.at[0], vec_recv.at[0])
    own_vec.start()
    for k in range(1, GROUP):
        vec_copy(k).start()
    old_vec = [pltpu.make_async_copy(src, lines.at[j, 0, pl.ds(0, src.shape[0])], line_sem.at[j])
               for j, src in enumerate((vec_master, vec_moment, vec_second))]
    for one in old_vec:
        one.start()

    def tick(u, carry):
        for c in range(3):
            @pl.when(u < chunks)
            def _():
                sum_a(c, u)
        for c in range(3):
            @pl.when((u >= 1) & (u < chunks + 1))
            def _():
                sum_b(c, u - 1)
        for c in range(3):
            @pl.when(u >= 2)
            def _():
                sum_c(c, u - 2)
        for c in range(3):
            @pl.when(u + 2 < chunks)
            def _():
                pack(c, u + 2)
                send_a(c, u + 2)
                load_after(c, u + 2)

        @pl.when(u == chunks // 2)
        def _():
            own_vec.wait()
            total = vec_in[0].astype(F32)
            for k in range(1, GROUP):
                vec_copy(k).wait()
                total = total + vec_in[k].astype(F32)
            padding = jnp.zeros((1, vec_total.shape[1] - total.shape[1]), F32)
            vec_total[...] = jnp.concatenate([total, padding], axis=1)
            square[0:1, :] += sum((total * total)[:, LANES * k:LANES * (k + 1)] for k in range(total.shape[1] // LANES))

        return carry

    lax.fori_loop(0, chunks + 2, tick, 0)

    for c in range(3):
        for t in range(chunks - PACK_SLOTS, chunks):
            for j in range(3):
                copy_a(c, t, j).wait_send()
    for k in range(1, GROUP):
        square_copy(k).start()

    pltpu.make_async_copy(state.at[pl.ds(0, share_rows)], state.at[pl.ds(0, share_rows)], send_c_sem).wait()
    for c in range(3):
        for t in range(chunks - 2, chunks):
            copy_b(c, t).wait_send()

    order = [(c, k) for k in range(parts) for c in range(3)]

    def place(c, k, which=0):
        return pl.ds(which * share_rows + (c * parts + k) * span, span)

    def master_load(n):
        return pltpu.make_async_copy(master.at[place(*order[n])], stage.at[n % 2], stage_sem.at[n % 2])

    def state_loads(c, k):
        return [pltpu.make_async_copy(src.at[place(c, k)], state.at[place(c, k, 1 + j)], state_sem.at[c, k, j])
                for j, src in enumerate((moment, second))]

    for n, (c, k) in enumerate(order):
        if n < 2:
            master_load(n).start()
        for one in state_loads(c, k):
            one.start()

    whole = square[...]
    for k in range(1, GROUP):
        square_copy(k).wait_recv()
        whole = whole + square_in[k]
    norm = jnp.sqrt(jnp.sum(whole, keepdims=True))
    clip_one = jnp.minimum(1.0, 1.0 / (norm + NORM_EPS))
    clip_coef = jnp.broadcast_to(clip_one, (1, LANES))

    def block(source, c, k):
        return aligned(source * share_rows + (c * parts + k) * span, span)

    def message(c, k, origin, step):
        here = block(flip(me, origin), c, k)
        return pltpu.make_async_remote_copy(
            src_ref=out.at[here], dst_ref=out.at[here],
            send_sem=send_sem, recv_sem=recv_sem.at[c, k, sum(origin) + step],
            device_id=(across(me, step),), device_id_type=MESH)

    def arrived(c, k, origin):
        pltpu.make_async_remote_copy(
            src_ref=out.at[block(me, c, k)], dst_ref=out.at[block(flip(me, origin), c, k)],
            send_sem=send_sem, recv_sem=recv_sem.at[c, k, sum(origin)],
            device_id=(across(me, 1),), device_id_type=MESH).wait_recv()

    def forward(c, k, origin, steps):
        arrived(c, k, origin)
        for step in steps:
            message(c, k, origin, step).start()

    step_blk = 48

    def update(n, c, k):
        def body(b, carry):
            first = (c * parts + k) * span + b * step_blk
            here, there, last = [aligned(first + j * share_rows, step_blk) for j in range(3)]
            p, m, v = adam_update(state[here, :], clip_coef, stage[n % 2, aligned(b * step_blk, step_blk), :],
                                  state[there, :], state[last, :], DECAY)
            state[here, :] = p
            state[there, :] = m
            state[last, :] = v
            out[aligned(me * share_rows + first, step_blk), :] = p.astype(BF16)
            return carry

        lax.fori_loop(0, span // step_blk, body, 0)

    for n, (c, k) in enumerate(order):
        master_load(n).wait()
        for one in state_loads(c, k):
            one.wait()
        update(n, c, k)
        if n + 2 < len(order):
            master_load(n + 2).start()
        for step in DIMS[c] + (1,):
            message(c, k, (), step).start()

    def share_copy(k, source):
        return small_copy(vec_share, vec_out.at[source], k, share_send, share_recv)

    width = vec_share.shape[1]
    for one in old_vec:
        one.wait()
    old = [lines[j][:, :width] for j in range(3)]
    fresh = adam_update(vec_total[...][:, :width], clip_one, *old, 0.0)
    for j in range(3):
        vec_state[j] = fresh[j]
    vec_share[...] = fresh[0].astype(BF16)
    vec_out[me] = fresh[0].astype(BF16)
    for k in range(1, GROUP):
        share_copy(k, me).start()

    for origin, steps in (((0,), (1, 2)), ((1,), (2,)), ((2,), ()), ((0, 1), (2,)), ((0, 2), ()), ((1, 2), ()), ((0, 1, 2), ())):
        for c in range(3):
            for k in range(parts):
                forward(c, k, tuple(DIMS[c][j] for j in origin), tuple(DIMS[c][j] for j in steps) + (1,))
    for mask in range(8):
        for c in range(3):
            for k in range(parts):
                arrived(c, k, tuple(STRIDES[j] for j in range(3) if mask // 2 ** j % 2) + (1,))
    for k in range(1, GROUP):
        square_copy(k).wait_send()
        share_copy(k, lax.rem(me + GROUP - k, GROUP)).wait()
    sent = pl.ds(0, (GROUP - 1) * share_rows)
    pltpu.make_async_copy(out.at[sent], out.at[sent], send_sem).wait()


def drain_kernel(pieces, weights, state, vec, vec_state, weights_out, master, moment, second,
                 vec_out, vec_master, vec_moment, vec_second, vec_flat, sem):
    copies = []
    share_rows = master.shape[0]
    for src, start, dst, count in ((weights, 0, weights_out, 4 * pieces), (state, 0, master, pieces),
                                   (state, share_rows, moment, pieces), (state, 2 * share_rows, second, pieces)):
        size = dst.shape[0] // count
        copies += [pltpu.make_async_copy(src.at[pl.ds(start + k * size, size)], dst.at[pl.ds(k * size, size)],
                                         sem.at[len(copies) + k]) for k in range(count)]
    copies += [pltpu.make_async_copy(vec_state.at[j, 0], dst, sem.at[len(copies) + j])
               for j, dst in enumerate((vec_master, vec_moment, vec_second))]
    for copy in copies:
        copy.start()
    vec_flat[...] = jnp.concatenate([vec[k].astype(F32).reshape(-1, LANES) for k in range(vec.shape[0])], axis=0).astype(BF16)
    copies.append(pltpu.make_async_copy(vec_flat, vec_out, sem.at[len(copies)]))
    copies[-1].start()
    for copy in copies:
        copy.wait()


def full_step(grad_mat, grad_vec, state, vec_state, chunks, parts):
    share_rows = grad_mat.shape[1] // GROUP // LANES
    rows = share_rows // (3 * chunks)
    span = share_rows // (3 * parts)
    width = grad_vec.shape[1] // GROUP
    vmem, anywhere = pl.BlockSpec(memory_space=pltpu.VMEM), pl.BlockSpec(memory_space=pl.ANY)
    dma = pltpu.SemaphoreType.DMA
    held = pl.pallas_call(
        functools.partial(step_kernel, chunks, rows, parts),
        out_shape=(pltpu.VMEM((GROUP * share_rows, LANES), BF16), pltpu.VMEM((3 * share_rows, LANES), F32),
                   pltpu.VMEM((GROUP, 1, width), BF16), pltpu.VMEM((3, 1, width), F32)),
        in_specs=[anywhere] * 8,
        out_specs=(vmem,) * 4,
        scratch_shapes=[
            pltpu.VMEM((3, GROUP, 1, rows * LANES), BF16),
            pltpu.VMEM((3, 2, 2 * rows, LANES), F32),
            pltpu.VMEM((2, span, LANES), F32),
            pltpu.VMEM((GROUP, 1, width), BF16),
            pltpu.VMEM((3, 1, -(-width // 1024) * 1024), F32),
            pltpu.VMEM((1, -(-width // 1024) * 1024), F32),
            pltpu.VMEM((1, width), BF16),
            pltpu.VMEM((8, LANES), F32),
            pltpu.VMEM((GROUP, 8, LANES), F32),
            dma((3,)), dma((3,)), dma((3, PACK_SLOTS, 3)), dma((3, chunks, 3)), dma((3, 2)), dma((3, chunks)), dma, dma((3, chunks)),
            dma((GROUP,)), dma((GROUP,)), dma((GROUP,)), dma((GROUP,)), dma((2,)), dma((3, parts, 2)),
            dma, dma((3, parts, GROUP)), dma((GROUP,)), dma((GROUP,)),
        ],
        compiler_params=pltpu.CompilerParams(collective_id=0, has_side_effects=True, vmem_limit_bytes=14 * 512 * 1024),
        name='full_step',
    )(grad_mat.reshape(GROUP, 3, chunks, 1, rows * LANES), grad_vec.reshape(GROUP, 1, width),
      *[x.reshape(share_rows, LANES) for x in state], *vec_state)
    pieces = 4
    states = jax.ShapeDtypeStruct((share_rows, LANES), F32)
    vectors = jax.ShapeDtypeStruct((width,), F32)
    weights, *rest = pl.pallas_call(
        functools.partial(drain_kernel, pieces),
        out_shape=(jax.ShapeDtypeStruct((GROUP * share_rows, LANES), BF16), states, states, states,
                   jax.ShapeDtypeStruct((GROUP * width // LANES, LANES), BF16), vectors, vectors, vectors),
        in_specs=[vmem] * 4,
        out_specs=(anywhere,) * 8,
        scratch_shapes=[pltpu.VMEM((GROUP * width // LANES, LANES), BF16), dma((7 * pieces + 4,))],
        compiler_params=pltpu.CompilerParams(vmem_limit_bytes=7 * 1024 * 1024),
        name='drain',
    )(*[pltpu.with_memory_space_constraint(x, pltpu.VMEM) for x in held])
    flat = [x.reshape(-1) for x in rest]
    return tuple(flat[:3] + flat[4:] + [weights.reshape(-1), flat[3]])


def solution(mesh):
    def local_step(grad_mat, grad_vec, master_mat, moment_mat, second_mat, master_vec, moment_vec, second_vec):
        return full_step(grad_mat, grad_vec, (master_mat, moment_mat, second_mat),
                         (master_vec, moment_vec, second_vec), 18, 4)

    row_spec = P('fsdp', None)
    flat_spec = P('fsdp')
    whole_spec = P()
    return jax.shard_map(local_step, mesh=mesh,
                         in_specs=(row_spec, row_spec) + (flat_spec,) * 6,
                         out_specs=(flat_spec,) * 6 + (whole_spec, whole_spec),
                         check_vma=False)
```

```python
import functools

import jax
import jax.numpy as jnp
from jax import lax
from jax.experimental import pallas as pl
from jax.experimental.pallas import tpu as pltpu
from jax.sharding import PartitionSpec as P

STEP = 4
LEARN_RATE = 1e-3
BETA_ONE = 0.9
BETA_TWO = 0.999
ADAM_EPS = 1e-8
DECAY = 0.01
NORM_EPS = 1e-6
FIX_ONE = 1.0 - BETA_ONE ** STEP
FIX_TWO = 1.0 - BETA_TWO ** STEP

MESH = pl.DeviceIdType.MESH
LANES = 128
GROUP = 16
STRIDES = (2, 4, 8)
DIMS = tuple(tuple(STRIDES[(c + j) % 3] for j in range(3)) for c in range(3))
PACK_SLOTS = 4
F32 = jnp.float32
BF16 = jnp.bfloat16


def adam_update(grad_sum, clip_coef, master, moment, second, decay):
    clip_grad = clip_coef * grad_sum
    new_moment = BETA_ONE * moment + (1.0 - BETA_ONE) * clip_grad
    new_second = BETA_TWO * second + (1.0 - BETA_TWO) * clip_grad * clip_grad
    step_dir = (new_moment / FIX_ONE) / (jnp.sqrt(new_second / FIX_TWO) + ADAM_EPS)
    new_master = master - LEARN_RATE * (step_dir + decay * master)
    return new_master, new_moment, new_second


def bit_of(index, stride):
    return lax.rem(lax.div(index, stride), 2)


def across(index, stride):
    return index + stride * (1 - 2 * bit_of(index, stride))


def flip(index, strides):
    for stride in strides:
        index = across(index, stride)
    return index


def aligned(start, size):
    return pl.ds(pl.multiple_of(start, 16), size)


def step_kernel(chunks, rows, parts, grad, gvec, master, moment, second, vec_master, vec_moment, vec_second,
                out, state, vec_out, vec_state,
                raw, send_b, stage, vec_in, lines, vec_total, vec_share, square, square_in,
                line_sem, raw_sem, send_a_sem, recv_a_sem, send_b_sem, recv_b_sem, send_c_sem, recv_c_sem,
                vec_send, vec_recv, square_send, square_recv, stage_sem, state_sem,
                send_sem, recv_sem, share_send, share_recv):
    me = lax.axis_index('fsdp')
    core = bit_of(me, 1)
    share_rows = 3 * chunks * rows
    span = share_rows // (3 * parts)

    def packed(c, t, quarter):
        return aligned(((c * PACK_SLOTS + lax.rem(t, PACK_SLOTS)) * 4 + quarter) * 4 * rows, 4 * rows)

    def landed(c, t, j):
        return aligned((3 * PACK_SLOTS * 4 + (c * chunks + t) * 3 + j) * 4 * rows, 4 * rows)

    def half_sums(c, t):
        return aligned(share_rows + (c * chunks + t) * 2 * rows, 2 * rows)

    def totals(c, t):
        return aligned((c * chunks + t) * rows, rows)

    def load(c, t):
        return pltpu.make_async_copy(grad.at[:, c, t], raw.at[c], raw_sem.at[c])

    def copy_a(c, t, j):
        d1 = DIMS[c][0]
        mine, other = bit_of(me, d1), across(me, d1)
        device, d1_bit, core_bit = ((across(me, 1), mine, 1 - core), (other, 1 - mine, core),
                                    (across(other, 1), 1 - mine, 1 - core))[j]
        return pltpu.make_async_remote_copy(
            src_ref=out.at[packed(c, t, 2 * d1_bit + core_bit)], dst_ref=out.at[landed(c, t, j)],
            send_sem=send_a_sem.at[c, lax.rem(t, PACK_SLOTS), j], recv_sem=recv_a_sem.at[c, t, j],
            device_id=(device,), device_id_type=MESH)

    def copy_b(c, t):
        s = lax.rem(t, 2)
        return pltpu.make_async_remote_copy(
            src_ref=send_b.at[c, s], dst_ref=state.at[half_sums(c, t)],
            send_sem=send_b_sem.at[c, s], recv_sem=recv_b_sem.at[c, t],
            device_id=(across(me, DIMS[c][1]),), device_id_type=MESH)

    def copy_c(c, t):
        away = 1 - bit_of(me, DIMS[c][2])
        source = aligned(share_rows + ((c * chunks + t) * 2 + away) * rows, rows)
        return pltpu.make_async_remote_copy(
            src_ref=state.at[source], dst_ref=state.at[totals(c, t)],
            send_sem=send_c_sem, recv_sem=recv_c_sem.at[c, t],
            device_id=(across(me, DIMS[c][2]),), device_id_type=MESH)

    blk = 192
    blocks = rows // blk

    def pack(c, t):
        load(c, t).wait()

        @pl.when(t >= PACK_SLOTS)
        def _():
            for j in range(3):
                copy_a(c, t - PACK_SLOTS, j).wait_send()

        base = (c * PACK_SLOTS + lax.rem(t, PACK_SLOTS)) * 16 * rows
        for share in range(GROUP):
            d1_bit, core_bit, d2_bit, d3_bit = [(share // d) % 2 for d in (DIMS[c][0], 1) + DIMS[c][1:]]
            place = 8 * d1_bit + 4 * core_bit + 2 * d2_bit + d3_bit

            def body(b, carry):
                columns = pl.ds(pl.multiple_of(b * blk * LANES, blk * LANES), blk * LANES)
                out[aligned(base + place * rows + b * blk, blk), :] = raw[c, share, :, columns].reshape(blk, LANES)
                return carry

            lax.fori_loop(0, blocks, body, 0)

    def send_a(c, t):
        for j in range(3):
            copy_a(c, t, j).start()

    def load_after(c, t):
        @pl.when(t + 1 < chunks)
        def _():
            load(c, t + 1).start()

    def local_sum(c, t, row):
        own = ((c * PACK_SLOTS + lax.rem(t, PACK_SLOTS)) * 4 + 2 * bit_of(me, DIMS[c][0]) + core) * 4 * rows
        others = [(3 * PACK_SLOTS * 4 + (c * chunks + t) * 3 + j) * 4 * rows for j in range(3)]
        one, two, three, four = [out[aligned(base + row, blk), :].astype(F32) for base in [own] + others]
        return (one + two) + (three + four)

    def sum_a(c, t):
        for j in range(3):
            copy_a(c, t, j).wait_recv()

        @pl.when(t >= 2)
        def _():
            copy_b(c, t - 2).wait_send()

        away = 1 - bit_of(me, DIMS[c][1])

        def body(b, carry):
            send_b[c, lax.rem(t, 2), aligned(b * blk, blk), :] = local_sum(c, t, away * 2 * rows + b * blk)
            return carry

        lax.fori_loop(0, 2 * blocks, body, 0)
        copy_b(c, t).start()

    def sum_b(c, t):
        copy_b(c, t).wait_recv()
        near, mine = bit_of(me, DIMS[c][1]), bit_of(me, DIMS[c][2])

        def add(k):
            def body(b, carry):
                held = aligned(share_rows + ((c * chunks + t) * 2 + k) * rows + b * blk, blk)
                state[held, :] = local_sum(c, t, (near * 2 + k) * rows + b * blk) + state[held, :]
                return carry

            lax.fori_loop(0, blocks, body, 0)

        add(1 - mine)
        copy_c(c, t).start()
        add(mine)

    def sum_c(c, t):
        copy_c(c, t).wait_recv()
        mine = bit_of(me, DIMS[c][2])

        def body(b, running):
            held = aligned(share_rows + ((c * chunks + t) * 2 + mine) * rows + b * blk, blk)
            here = aligned((c * chunks + t) * rows + b * blk, blk)
            total = state[held, :] + state[here, :]
            state[here, :] = total
            return running + jnp.sum((total * total).reshape(blk // 8, 8, LANES), axis=0)

        square[...] += lax.fori_loop(0, blocks, body, jnp.zeros((8, LANES), F32))

    def small_copy(src, dst, k, sends, recvs):
        return pltpu.make_async_remote_copy(
            src_ref=src, dst_ref=dst, send_sem=sends.at[k], recv_sem=recvs.at[k],
            device_id=(lax.rem(me + k, GROUP),), device_id_type=MESH)

    def vec_copy(k):
        return small_copy(gvec.at[lax.rem(me + k, GROUP)], vec_in.at[k], k, vec_send, vec_recv)

    def square_copy(k):
        return small_copy(square, square_in.at[k], k, square_send, square_recv)

    barrier = pltpu.get_barrier_semaphore()
    for k in range(1, GROUP):
        pl.semaphore_signal(barrier, inc=1, device_id=(lax.rem(me + k, GROUP),), device_id_type=MESH)
    for c in range(3):
        load(c, 0).start()
    square[...] = jnp.zeros_like(square)
    pack(0, 0)
    pl.semaphore_wait(barrier, GROUP - 1)
    send_a(0, 0)
    load_after(0, 0)
    for t in range(2):
        for c in range(1 if t == 0 else 0, 3):
            pack(c, t)
            send_a(c, t)
            load_after(c, t)
    own_vec = pltpu.make_async_copy(gvec.at[me], vec_in.at[0], vec_recv.at[0])
    own_vec.start()
    for k in range(1, GROUP):
        vec_copy(k).start()
    old_vec = [pltpu.make_async_copy(src, lines.at[j, 0, pl.ds(0, src.shape[0])], line_sem.at[j])
               for j, src in enumerate((vec_master, vec_moment, vec_second))]
    for one in old_vec:
        one.start()

    def tick(u, carry):
        for c in range(3):
            @pl.when(u < chunks)
            def _():
                sum_a(c, u)
        for c in range(3):
            @pl.when((u >= 1) & (u < chunks + 1))
            def _():
                sum_b(c, u - 1)
        for c in range(3):
            @pl.when(u >= 2)
            def _():
                sum_c(c, u - 2)
        for c in range(3):
            @pl.when(u + 2 < chunks)
            def _():
                pack(c, u + 2)
                send_a(c, u + 2)
                load_after(c, u + 2)

        @pl.when(u == chunks // 2)
        def _():
            own_vec.wait()
            total = vec_in[0].astype(F32)
            for k in range(1, GROUP):
                vec_copy(k).wait()
                total = total + vec_in[k].astype(F32)
            padding = jnp.zeros((1, vec_total.shape[1] - total.shape[1]), F32)
            vec_total[...] = jnp.concatenate([total, padding], axis=1)
            square[0:1, :] += sum((total * total)[:, LANES * k:LANES * (k + 1)] for k in range(total.shape[1] // LANES))

        return carry

    lax.fori_loop(0, chunks + 2, tick, 0)

    for c in range(3):
        for t in range(chunks - PACK_SLOTS, chunks):
            for j in range(3):
                copy_a(c, t, j).wait_send()
    for k in range(1, GROUP):
        square_copy(k).start()

    pltpu.make_async_copy(state.at[pl.ds(0, share_rows)], state.at[pl.ds(0, share_rows)], send_c_sem).wait()
    for c in range(3):
        for t in range(chunks - 2, chunks):
            copy_b(c, t).wait_send()

    order = [(c, k) for k in range(parts) for c in range(3)]

    def place(c, k, which=0):
        return pl.ds(which * share_rows + (c * parts + k) * span, span)

    def master_load(n):
        return pltpu.make_async_copy(master.at[place(*order[n])], stage.at[n % 2], stage_sem.at[n % 2])

    def state_loads(c, k):
        return [pltpu.make_async_copy(src.at[place(c, k)], state.at[place(c, k, 1 + j)], state_sem.at[c, k, j])
                for j, src in enumerate((moment, second))]

    for n, (c, k) in enumerate(order):
        if n < 2:
            master_load(n).start()
        for one in state_loads(c, k):
            one.start()

    whole = square[...]
    for k in range(1, GROUP):
        square_copy(k).wait_recv()
        whole = whole + square_in[k]
    norm = jnp.sqrt(jnp.sum(whole, keepdims=True))
    clip_one = jnp.minimum(1.0, 1.0 / (norm + NORM_EPS))
    clip_coef = jnp.broadcast_to(clip_one, (1, LANES))

    def block(source, c, k):
        return aligned(source * share_rows + (c * parts + k) * span, span)

    def message(c, k, origin, step):
        here = block(flip(me, origin), c, k)
        return pltpu.make_async_remote_copy(
            src_ref=out.at[here], dst_ref=out.at[here],
            send_sem=send_sem, recv_sem=recv_sem.at[c, k, sum(origin) + step],
            device_id=(across(me, step),), device_id_type=MESH)

    def arrived(c, k, origin):
        pltpu.make_async_remote_copy(
            src_ref=out.at[block(me, c, k)], dst_ref=out.at[block(flip(me, origin), c, k)],
            send_sem=send_sem, recv_sem=recv_sem.at[c, k, sum(origin)],
            device_id=(across(me, 1),), device_id_type=MESH).wait_recv()

    def forward(c, k, origin, steps):
        arrived(c, k, origin)
        for step in steps:
            message(c, k, origin, step).start()

    step_blk = 96

    def update(n, c, k):
        def body(b, carry):
            first = (c * parts + k) * span + b * step_blk
            here, there, last = [aligned(first + j * share_rows, step_blk) for j in range(3)]
            p, m, v = adam_update(state[here, :], clip_coef, stage[n % 2, aligned(b * step_blk, step_blk), :],
                                  state[there, :], state[last, :], DECAY)
            state[here, :] = p
            state[there, :] = m
            state[last, :] = v
            out[aligned(me * share_rows + first, step_blk), :] = p.astype(BF16)
            return carry

        lax.fori_loop(0, span // step_blk, body, 0)

    for n, (c, k) in enumerate(order):
        master_load(n).wait()
        for one in state_loads(c, k):
            one.wait()
        update(n, c, k)
        if n + 2 < len(order):
            master_load(n + 2).start()
        for step in DIMS[c] + (1,):
            message(c, k, (), step).start()

    def share_copy(k, source):
        return small_copy(vec_share, vec_out.at[source], k, share_send, share_recv)

    width = vec_share.shape[1]
    for one in old_vec:
        one.wait()
    old = [lines[j][:, :width] for j in range(3)]
    fresh = adam_update(vec_total[...][:, :width], clip_one, *old, 0.0)
    for j in range(3):
        vec_state[j] = fresh[j]
    vec_share[...] = fresh[0].astype(BF16)
    vec_out[me] = fresh[0].astype(BF16)
    for k in range(1, GROUP):
        share_copy(k, me).start()

    onward = {(0,): (1, 2), (1,): (2,), (0, 1): (2,)}
    for phase in (((0,), (1,), (2,)), ((0, 1), (0, 2), (1, 2)), ((0, 1, 2),)):
        for k in range(parts):
            for c in range(3):
                for origin in phase:
                    steps = onward.get(origin, ())
                    forward(c, k, tuple(DIMS[c][j] for j in origin), tuple(DIMS[c][j] for j in steps) + (1,))
    for mask in range(8):
        for k in range(parts):
            for c in range(3):
                arrived(c, k, tuple(STRIDES[j] for j in range(3) if mask // 2 ** j % 2) + (1,))
    for k in range(1, GROUP):
        square_copy(k).wait_send()
        share_copy(k, lax.rem(me + GROUP - k, GROUP)).wait()
    sent = pl.ds(0, (GROUP - 1) * share_rows)
    pltpu.make_async_copy(out.at[sent], out.at[sent], send_sem).wait()


def drain_kernel(pieces, weights, state, vec, vec_state, weights_out, master, moment, second,
                 vec_out, vec_master, vec_moment, vec_second, vec_flat, sem):
    copies = []
    share_rows = master.shape[0]
    for src, start, dst, count in ((weights, 0, weights_out, 4 * pieces), (state, 0, master, pieces),
                                   (state, share_rows, moment, pieces), (state, 2 * share_rows, second, pieces)):
        size = dst.shape[0] // count
        copies += [pltpu.make_async_copy(src.at[pl.ds(start + k * size, size)], dst.at[pl.ds(k * size, size)],
                                         sem.at[len(copies) + k]) for k in range(count)]
    copies += [pltpu.make_async_copy(vec_state.at[j, 0], dst, sem.at[len(copies) + j])
               for j, dst in enumerate((vec_master, vec_moment, vec_second))]
    for copy in copies:
        copy.start()
    vec_flat[...] = jnp.concatenate([vec[k].astype(F32).reshape(-1, LANES) for k in range(vec.shape[0])], axis=0).astype(BF16)
    copies.append(pltpu.make_async_copy(vec_flat, vec_out, sem.at[len(copies)]))
    copies[-1].start()
    for copy in copies:
        copy.wait()


def full_step(grad_mat, grad_vec, state, vec_state, chunks, parts):
    share_rows = grad_mat.shape[1] // GROUP // LANES
    rows = share_rows // (3 * chunks)
    span = share_rows // (3 * parts)
    width = grad_vec.shape[1] // GROUP
    vmem, anywhere = pl.BlockSpec(memory_space=pltpu.VMEM), pl.BlockSpec(memory_space=pl.ANY)
    dma = pltpu.SemaphoreType.DMA
    held = pl.pallas_call(
        functools.partial(step_kernel, chunks, rows, parts),
        out_shape=(pltpu.VMEM((GROUP * share_rows, LANES), BF16), pltpu.VMEM((3 * share_rows, LANES), F32),
                   pltpu.VMEM((GROUP, 1, width), BF16), pltpu.VMEM((3, 1, width), F32)),
        in_specs=[anywhere] * 8,
        out_specs=(vmem,) * 4,
        scratch_shapes=[
            pltpu.VMEM((3, GROUP, 1, rows * LANES), BF16),
            pltpu.VMEM((3, 2, 2 * rows, LANES), F32),
            pltpu.VMEM((2, span, LANES), F32),
            pltpu.VMEM((GROUP, 1, width), BF16),
            pltpu.VMEM((3, 1, -(-width // 1024) * 1024), F32),
            pltpu.VMEM((1, -(-width // 1024) * 1024), F32),
            pltpu.VMEM((1, width), BF16),
            pltpu.VMEM((8, LANES), F32),
            pltpu.VMEM((GROUP, 8, LANES), F32),
            dma((3,)), dma((3,)), dma((3, PACK_SLOTS, 3)), dma((3, chunks, 3)), dma((3, 2)), dma((3, chunks)), dma, dma((3, chunks)),
            dma((GROUP,)), dma((GROUP,)), dma((GROUP,)), dma((GROUP,)), dma((2,)), dma((3, parts, 2)),
            dma, dma((3, parts, GROUP)), dma((GROUP,)), dma((GROUP,)),
        ],
        compiler_params=pltpu.CompilerParams(collective_id=0, has_side_effects=True, vmem_limit_bytes=14 * 512 * 1024),
        name='full_step',
    )(grad_mat.reshape(GROUP, 3, chunks, 1, rows * LANES), grad_vec.reshape(GROUP, 1, width),
      *[x.reshape(share_rows, LANES) for x in state], *vec_state)
    pieces = 4
    states = jax.ShapeDtypeStruct((share_rows, LANES), F32)
    vectors = jax.ShapeDtypeStruct((width,), F32)
    weights, *rest = pl.pallas_call(
        functools.partial(drain_kernel, pieces),
        out_shape=(jax.ShapeDtypeStruct((GROUP * share_rows, LANES), BF16), states, states, states,
                   jax.ShapeDtypeStruct((GROUP * width // LANES, LANES), BF16), vectors, vectors, vectors),
        in_specs=[vmem] * 4,
        out_specs=(anywhere,) * 8,
        scratch_shapes=[pltpu.VMEM((GROUP * width // LANES, LANES), BF16), dma((7 * pieces + 4,))],
        compiler_params=pltpu.CompilerParams(vmem_limit_bytes=7 * 1024 * 1024),
        name='drain',
    )(*[pltpu.with_memory_space_constraint(x, pltpu.VMEM) for x in held])
    flat = [x.reshape(-1) for x in rest]
    return tuple(flat[:3] + flat[4:] + [weights.reshape(-1), flat[3]])


def solution(mesh):
    def local_step(grad_mat, grad_vec, master_mat, moment_mat, second_mat, master_vec, moment_vec, second_vec):
        return full_step(grad_mat, grad_vec, (master_mat, moment_mat, second_mat),
                         (master_vec, moment_vec, second_vec), 18, 4)

    row_spec = P('fsdp', None)
    flat_spec = P('fsdp')
    whole_spec = P()
    return jax.shard_map(local_step, mesh=mesh,
                         in_specs=(row_spec, row_spec) + (flat_spec,) * 6,
                         out_specs=(flat_spec,) * 6 + (whole_spec, whole_spec),
                         check_vma=False)
```

```python
import functools

import jax
import jax.numpy as jnp
from jax import lax
from jax.experimental import pallas as pl
from jax.experimental.pallas import tpu as pltpu
from jax.sharding import PartitionSpec as P

STEP = 4
LEARN_RATE = 1e-3
BETA_ONE = 0.9
BETA_TWO = 0.999
ADAM_EPS = 1e-8
DECAY = 0.01
NORM_EPS = 1e-6
FIX_ONE = 1.0 - BETA_ONE ** STEP
FIX_TWO = 1.0 - BETA_TWO ** STEP

MESH = pl.DeviceIdType.MESH
LANES = 128
GROUP = 16
STRIDES = (2, 4, 8)
DIMS = tuple(tuple(STRIDES[(c + j) % 3] for j in range(3)) for c in range(3))
PACK_SLOTS = 4
F32 = jnp.float32
BF16 = jnp.bfloat16


def adam_update(grad_sum, clip_coef, master, moment, second, decay):
    clip_grad = clip_coef * grad_sum
    new_moment = BETA_ONE * moment + (1.0 - BETA_ONE) * clip_grad
    new_second = BETA_TWO * second + (1.0 - BETA_TWO) * clip_grad * clip_grad
    step_dir = (new_moment / FIX_ONE) / (jnp.sqrt(new_second / FIX_TWO) + ADAM_EPS)
    new_master = master - LEARN_RATE * (step_dir + decay * master)
    return new_master, new_moment, new_second


def bit_of(index, stride):
    return lax.rem(lax.div(index, stride), 2)


def across(index, stride):
    return index + stride * (1 - 2 * bit_of(index, stride))


def flip(index, strides):
    for stride in strides:
        index = across(index, stride)
    return index


def aligned(start, size):
    return pl.ds(pl.multiple_of(start, 16), size)


def step_kernel(chunks, rows, parts, grad, gvec, master, moment, second, vec_master, vec_moment, vec_second,
                out, state, vec_out, vec_state,
                raw, send_b, stage, vec_in, lines, vec_total, vec_share, square, square_in,
                line_sem, raw_sem, send_a_sem, recv_a_sem, send_b_sem, recv_b_sem, send_c_sem, recv_c_sem,
                vec_send, vec_recv, square_send, square_recv, stage_sem, state_sem,
                send_sem, recv_sem, share_send, share_recv):
    me = lax.axis_index('fsdp')
    core = bit_of(me, 1)
    share_rows = 3 * chunks * rows
    span = share_rows // (3 * parts)

    def packed(c, t, quarter):
        return aligned(((c * PACK_SLOTS + lax.rem(t, PACK_SLOTS)) * 4 + quarter) * 4 * rows, 4 * rows)

    def landed(c, t, j):
        return aligned((3 * PACK_SLOTS * 4 + (c * chunks + t) * 3 + j) * 4 * rows, 4 * rows)

    def half_sums(c, t):
        return aligned(share_rows + (c * chunks + t) * 2 * rows, 2 * rows)

    def totals(c, t):
        return aligned((c * chunks + t) * rows, rows)

    def load(c, t):
        return pltpu.make_async_copy(grad.at[:, c, t], raw.at[c], raw_sem.at[c])

    def copy_a(c, t, j):
        d1 = DIMS[c][0]
        mine, other = bit_of(me, d1), across(me, d1)
        device, d1_bit, core_bit = ((across(me, 1), mine, 1 - core), (other, 1 - mine, core),
                                    (across(other, 1), 1 - mine, 1 - core))[j]
        return pltpu.make_async_remote_copy(
            src_ref=out.at[packed(c, t, 2 * d1_bit + core_bit)], dst_ref=out.at[landed(c, t, j)],
            send_sem=send_a_sem.at[c, lax.rem(t, PACK_SLOTS), j], recv_sem=recv_a_sem.at[c, t, j],
            device_id=(device,), device_id_type=MESH)

    def copy_b(c, t):
        s = lax.rem(t, 2)
        return pltpu.make_async_remote_copy(
            src_ref=send_b.at[c, s], dst_ref=state.at[half_sums(c, t)],
            send_sem=send_b_sem.at[c, s], recv_sem=recv_b_sem.at[c, t],
            device_id=(across(me, DIMS[c][1]),), device_id_type=MESH)

    def copy_c(c, t):
        away = 1 - bit_of(me, DIMS[c][2])
        source = aligned(share_rows + ((c * chunks + t) * 2 + away) * rows, rows)
        return pltpu.make_async_remote_copy(
            src_ref=state.at[source], dst_ref=state.at[totals(c, t)],
            send_sem=send_c_sem, recv_sem=recv_c_sem.at[c, t],
            device_id=(across(me, DIMS[c][2]),), device_id_type=MESH)

    blk = 192
    blocks = rows // blk

    def pack(c, t):
        load(c, t).wait()

        @pl.when(t >= PACK_SLOTS)
        def _():
            for j in range(3):
                copy_a(c, t - PACK_SLOTS, j).wait_send()

        base = (c * PACK_SLOTS + lax.rem(t, PACK_SLOTS)) * 16 * rows
        for share in range(GROUP):
            d1_bit, core_bit, d2_bit, d3_bit = [(share // d) % 2 for d in (DIMS[c][0], 1) + DIMS[c][1:]]
            place = 8 * d1_bit + 4 * core_bit + 2 * d2_bit + d3_bit

            def body(b, carry):
                columns = pl.ds(pl.multiple_of(b * blk * LANES, blk * LANES), blk * LANES)
                out[aligned(base + place * rows + b * blk, blk), :] = raw[c, share, :, columns].reshape(blk, LANES)
                return carry

            lax.fori_loop(0, blocks, body, 0)

    def pack_quarter(c, j):
        d1, d2, d3 = DIMS[c]
        mine = bit_of(me, d1)
        d1_bit, core_bit = ((mine, 1 - core), (1 - mine, core), (1 - mine, 1 - core), (mine, core))[j]
        for part in range(4):
            share = d1_bit * d1 + core_bit + part // 2 * d2 + part % 2 * d3
            first = ((c * PACK_SLOTS * 4 + 2 * d1_bit + core_bit) * 4 + part) * rows

            def body(b, carry):
                columns = pl.ds(pl.multiple_of(b * blk * LANES, blk * LANES), blk * LANES)
                out[aligned(first + b * blk, blk), :] = raw[c, share, :, columns].reshape(blk, LANES)
                return carry

            lax.fori_loop(0, blocks, body, 0)

    def send_a(c, t):
        for j in range(3):
            copy_a(c, t, j).start()

    def load_after(c, t):
        @pl.when(t + 1 < chunks)
        def _():
            load(c, t + 1).start()

    def local_sum(c, t, row):
        own = ((c * PACK_SLOTS + lax.rem(t, PACK_SLOTS)) * 4 + 2 * bit_of(me, DIMS[c][0]) + core) * 4 * rows
        others = [(3 * PACK_SLOTS * 4 + (c * chunks + t) * 3 + j) * 4 * rows for j in range(3)]
        one, two, three, four = [out[aligned(base + row, blk), :].astype(F32) for base in [own] + others]
        return (one + two) + (three + four)

    def sum_a(c, t):
        for j in range(3):
            copy_a(c, t, j).wait_recv()

        @pl.when(t >= 2)
        def _():
            copy_b(c, t - 2).wait_send()

        away = 1 - bit_of(me, DIMS[c][1])

        def body(b, carry):
            send_b[c, lax.rem(t, 2), aligned(b * blk, blk), :] = local_sum(c, t, away * 2 * rows + b * blk)
            return carry

        lax.fori_loop(0, 2 * blocks, body, 0)
        copy_b(c, t).start()

    def sum_b(c, t):
        copy_b(c, t).wait_recv()
        near, mine = bit_of(me, DIMS[c][1]), bit_of(me, DIMS[c][2])

        def add(k):
            def body(b, carry):
                held = aligned(share_rows + ((c * chunks + t) * 2 + k) * rows + b * blk, blk)
                state[held, :] = local_sum(c, t, (near * 2 + k) * rows + b * blk) + state[held, :]
                return carry

            lax.fori_loop(0, blocks, body, 0)

        add(1 - mine)
        copy_c(c, t).start()
        add(mine)

    def sum_c(c, t):
        copy_c(c, t).wait_recv()
        mine = bit_of(me, DIMS[c][2])

        def body(b, running):
            held = aligned(share_rows + ((c * chunks + t) * 2 + mine) * rows + b * blk, blk)
            here = aligned((c * chunks + t) * rows + b * blk, blk)
            total = state[held, :] + state[here, :]
            state[here, :] = total
            return running + jnp.sum((total * total).reshape(blk // 8, 8, LANES), axis=0)

        square[...] += lax.fori_loop(0, blocks, body, jnp.zeros((8, LANES), F32))

    def small_copy(src, dst, k, sends, recvs):
        return pltpu.make_async_remote_copy(
            src_ref=src, dst_ref=dst, send_sem=sends.at[k], recv_sem=recvs.at[k],
            device_id=(lax.rem(me + k, GROUP),), device_id_type=MESH)

    def vec_copy(k):
        return small_copy(gvec.at[lax.rem(me + k, GROUP)], vec_in.at[k], k, vec_send, vec_recv)

    def square_copy(k):
        return small_copy(square, square_in.at[k], k, square_send, square_recv)

    barrier = pltpu.get_barrier_semaphore()
    for k in range(1, GROUP):
        pl.semaphore_signal(barrier, inc=1, device_id=(lax.rem(me + k, GROUP),), device_id_type=MESH)
    for c in range(3):
        load(c, 0).start()
    square[...] = jnp.zeros_like(square)
    for c in range(3):
        load(c, 0).wait()
        pack_quarter(c, 1)
    pl.semaphore_wait(barrier, GROUP - 1)
    for c in range(3):
        copy_a(c, 0, 1).start()
    for j in (2, 0):
        for c in range(3):
            pack_quarter(c, j)
            copy_a(c, 0, j).start()
    for c in range(3):
        pack_quarter(c, 3)
        load_after(c, 0)
    for c in range(3):
        pack(c, 1)
        send_a(c, 1)
        load_after(c, 1)
    own_vec = pltpu.make_async_copy(gvec.at[me], vec_in.at[0], vec_recv.at[0])
    own_vec.start()
    for k in range(1, GROUP):
        vec_copy(k).start()
    old_vec = [pltpu.make_async_copy(src, lines.at[j, 0, pl.ds(0, src.shape[0])], line_sem.at[j])
               for j, src in enumerate((vec_master, vec_moment, vec_second))]
    for one in old_vec:
        one.start()

    def tick(u, carry):
        for c in range(3):
            @pl.when(u < chunks)
            def _():
                sum_a(c, u)
        for c in range(3):
            @pl.when((u >= 1) & (u < chunks + 1))
            def _():
                sum_b(c, u - 1)
        for c in range(3):
            @pl.when(u >= 2)
            def _():
                sum_c(c, u - 2)
        for c in range(3):
            @pl.when(u + 2 < chunks)
            def _():
                pack(c, u + 2)
                send_a(c, u + 2)
                load_after(c, u + 2)

        @pl.when(u == chunks // 2)
        def _():
            own_vec.wait()
            total = vec_in[0].astype(F32)
            for k in range(1, GROUP):
                vec_copy(k).wait()
                total = total + vec_in[k].astype(F32)
            padding = jnp.zeros((1, vec_total.shape[1] - total.shape[1]), F32)
            vec_total[...] = jnp.concatenate([total, padding], axis=1)
            square[0:1, :] += sum((total * total)[:, LANES * k:LANES * (k + 1)] for k in range(total.shape[1] // LANES))

        return carry

    lax.fori_loop(0, chunks + 2, tick, 0)

    for c in range(3):
        for t in range(chunks - PACK_SLOTS, chunks):
            for j in range(3):
                copy_a(c, t, j).wait_send()
    for k in range(1, GROUP):
        square_copy(k).start()

    pltpu.make_async_copy(state.at[pl.ds(0, share_rows)], state.at[pl.ds(0, share_rows)], send_c_sem).wait()
    for c in range(3):
        for t in range(chunks - 2, chunks):
            copy_b(c, t).wait_send()

    order = [(c, k) for k in range(parts) for c in range(3)]

    def place(c, k, which=0):
        return pl.ds(which * share_rows + (c * parts + k) * span, span)

    def master_load(n):
        return pltpu.make_async_copy(master.at[place(*order[n])], stage.at[n % 2], stage_sem.at[n % 2])

    def state_loads(c, k):
        return [pltpu.make_async_copy(src.at[place(c, k)], state.at[place(c, k, 1 + j)], state_sem.at[c, k, j])
                for j, src in enumerate((moment, second))]

    for n, (c, k) in enumerate(order):
        if n < 2:
            master_load(n).start()
        for one in state_loads(c, k):
            one.start()

    whole = square[...]
    for k in range(1, GROUP):
        square_copy(k).wait_recv()
        whole = whole + square_in[k]
    norm = jnp.sqrt(jnp.sum(whole, keepdims=True))
    clip_one = jnp.minimum(1.0, 1.0 / (norm + NORM_EPS))
    clip_coef = jnp.broadcast_to(clip_one, (1, LANES))

    def block(source, c, k):
        return aligned(source * share_rows + (c * parts + k) * span, span)

    def message(c, k, origin, step):
        here = block(flip(me, origin), c, k)
        return pltpu.make_async_remote_copy(
            src_ref=out.at[here], dst_ref=out.at[here],
            send_sem=send_sem, recv_sem=recv_sem.at[c, k, sum(origin) + step],
            device_id=(across(me, step),), device_id_type=MESH)

    def arrived(c, k, origin):
        pltpu.make_async_remote_copy(
            src_ref=out.at[block(me, c, k)], dst_ref=out.at[block(flip(me, origin), c, k)],
            send_sem=send_sem, recv_sem=recv_sem.at[c, k, sum(origin)],
            device_id=(across(me, 1),), device_id_type=MESH).wait_recv()

    def forward(c, k, origin, steps):
        arrived(c, k, origin)
        for step in steps:
            message(c, k, origin, step).start()

    step_blk = 96

    def update(n, c, k):
        def body(b, carry):
            first = (c * parts + k) * span + b * step_blk
            here, there, last = [aligned(first + j * share_rows, step_blk) for j in range(3)]
            p, m, v = adam_update(state[here, :], clip_coef, stage[n % 2, aligned(b * step_blk, step_blk), :],
                                  state[there, :], state[last, :], DECAY)
            state[here, :] = p
            state[there, :] = m
            state[last, :] = v
            out[aligned(me * share_rows + first, step_blk), :] = p.astype(BF16)
            return carry

        lax.fori_loop(0, span // step_blk, body, 0)

    for n, (c, k) in enumerate(order):
        master_load(n).wait()
        for one in state_loads(c, k):
            one.wait()
        update(n, c, k)
        if n + 2 < len(order):
            master_load(n + 2).start()
        for step in DIMS[c] + (1,):
            message(c, k, (), step).start()

    def share_copy(k, source):
        return small_copy(vec_share, vec_out.at[source], k, share_send, share_recv)

    width = vec_share.shape[1]
    for one in old_vec:
        one.wait()
    old = [lines[j][:, :width] for j in range(3)]
    fresh = adam_update(vec_total[...][:, :width], clip_one, *old, 0.0)
    for j in range(3):
        vec_state[j] = fresh[j]
    vec_share[...] = fresh[0].astype(BF16)
    vec_out[me] = fresh[0].astype(BF16)
    for k in range(1, GROUP):
        share_copy(k, me).start()

    onward = {(0,): (1, 2), (1,): (2,), (0, 1): (2,)}
    for phase in (((0,), (1,), (2,)), ((0, 1), (0, 2), (1, 2)), ((0, 1, 2),)):
        for k in range(parts):
            for c in range(3):
                for origin in phase:
                    steps = onward.get(origin, ())
                    forward(c, k, tuple(DIMS[c][j] for j in origin), tuple(DIMS[c][j] for j in steps) + (1,))
    for mask in range(8):
        for k in range(parts):
            for c in range(3):
                arrived(c, k, tuple(STRIDES[j] for j in range(3) if mask // 2 ** j % 2) + (1,))
    for k in range(1, GROUP):
        square_copy(k).wait_send()
        share_copy(k, lax.rem(me + GROUP - k, GROUP)).wait()
    sent = pl.ds(0, (GROUP - 1) * share_rows)
    pltpu.make_async_copy(out.at[sent], out.at[sent], send_sem).wait()


def drain_kernel(pieces, weights, state, vec, vec_state, weights_out, master, moment, second,
                 vec_out, vec_master, vec_moment, vec_second, vec_flat, sem):
    copies = []
    share_rows = master.shape[0]
    for src, start, dst, count in ((weights, 0, weights_out, 4 * pieces), (state, 0, master, pieces),
                                   (state, share_rows, moment, pieces), (state, 2 * share_rows, second, pieces)):
        size = dst.shape[0] // count
        copies += [pltpu.make_async_copy(src.at[pl.ds(start + k * size, size)], dst.at[pl.ds(k * size, size)],
                                         sem.at[len(copies) + k]) for k in range(count)]
    copies += [pltpu.make_async_copy(vec_state.at[j, 0], dst, sem.at[len(copies) + j])
               for j, dst in enumerate((vec_master, vec_moment, vec_second))]
    for copy in copies:
        copy.start()
    vec_flat[...] = jnp.concatenate([vec[k].astype(F32).reshape(-1, LANES) for k in range(vec.shape[0])], axis=0).astype(BF16)
    copies.append(pltpu.make_async_copy(vec_flat, vec_out, sem.at[len(copies)]))
    copies[-1].start()
    for copy in copies:
        copy.wait()


def full_step(grad_mat, grad_vec, state, vec_state, chunks, parts):
    share_rows = grad_mat.shape[1] // GROUP // LANES
    rows = share_rows // (3 * chunks)
    span = share_rows // (3 * parts)
    width = grad_vec.shape[1] // GROUP
    vmem, anywhere = pl.BlockSpec(memory_space=pltpu.VMEM), pl.BlockSpec(memory_space=pl.ANY)
    dma = pltpu.SemaphoreType.DMA
    held = pl.pallas_call(
        functools.partial(step_kernel, chunks, rows, parts),
        out_shape=(pltpu.VMEM((GROUP * share_rows, LANES), BF16), pltpu.VMEM((3 * share_rows, LANES), F32),
                   pltpu.VMEM((GROUP, 1, width), BF16), pltpu.VMEM((3, 1, width), F32)),
        in_specs=[anywhere] * 8,
        out_specs=(vmem,) * 4,
        scratch_shapes=[
            pltpu.VMEM((3, GROUP, 1, rows * LANES), BF16),
            pltpu.VMEM((3, 2, 2 * rows, LANES), F32),
            pltpu.VMEM((2, span, LANES), F32),
            pltpu.VMEM((GROUP, 1, width), BF16),
            pltpu.VMEM((3, 1, -(-width // 1024) * 1024), F32),
            pltpu.VMEM((1, -(-width // 1024) * 1024), F32),
            pltpu.VMEM((1, width), BF16),
            pltpu.VMEM((8, LANES), F32),
            pltpu.VMEM((GROUP, 8, LANES), F32),
            dma((3,)), dma((3,)), dma((3, PACK_SLOTS, 3)), dma((3, chunks, 3)), dma((3, 2)), dma((3, chunks)), dma, dma((3, chunks)),
            dma((GROUP,)), dma((GROUP,)), dma((GROUP,)), dma((GROUP,)), dma((2,)), dma((3, parts, 2)),
            dma, dma((3, parts, GROUP)), dma((GROUP,)), dma((GROUP,)),
        ],
        compiler_params=pltpu.CompilerParams(collective_id=0, has_side_effects=True, vmem_limit_bytes=14 * 512 * 1024),
        name='full_step',
    )(grad_mat.reshape(GROUP, 3, chunks, 1, rows * LANES), grad_vec.reshape(GROUP, 1, width),
      *[x.reshape(share_rows, LANES) for x in state], *vec_state)
    pieces = 4
    states = jax.ShapeDtypeStruct((share_rows, LANES), F32)
    vectors = jax.ShapeDtypeStruct((width,), F32)
    weights, *rest = pl.pallas_call(
        functools.partial(drain_kernel, pieces),
        out_shape=(jax.ShapeDtypeStruct((GROUP * share_rows, LANES), BF16), states, states, states,
                   jax.ShapeDtypeStruct((GROUP * width // LANES, LANES), BF16), vectors, vectors, vectors),
        in_specs=[vmem] * 4,
        out_specs=(anywhere,) * 8,
        scratch_shapes=[pltpu.VMEM((GROUP * width // LANES, LANES), BF16), dma((7 * pieces + 4,))],
        compiler_params=pltpu.CompilerParams(vmem_limit_bytes=7 * 1024 * 1024),
        name='drain',
    )(*[pltpu.with_memory_space_constraint(x, pltpu.VMEM) for x in held])
    flat = [x.reshape(-1) for x in rest]
    return tuple(flat[:3] + flat[4:] + [weights.reshape(-1), flat[3]])


def solution(mesh):
    def local_step(grad_mat, grad_vec, master_mat, moment_mat, second_mat, master_vec, moment_vec, second_vec):
        return full_step(grad_mat, grad_vec, (master_mat, moment_mat, second_mat),
                         (master_vec, moment_vec, second_vec), 18, 4)

    row_spec = P('fsdp', None)
    flat_spec = P('fsdp')
    whole_spec = P()
    return jax.shard_map(local_step, mesh=mesh,
                         in_specs=(row_spec, row_spec) + (flat_spec,) * 6,
                         out_specs=(flat_spec,) * 6 + (whole_spec, whole_spec),
                         check_vma=False)
```
